32 devices in a mesh: tp: 4 (over z), dp: 8 (over y, x, core).
Axes of the slice: x: 2, y: 2, z: 4, core: 2. Of those that a mesh axis runs over, the one named last changes fastest.
Arguments:
- design: float32 [65536, 1536], P('dp', 'tp')
- target: float32 [65536], P('dp')
- ridge: float32 [], replicated
Outputs:
- output 1: float32 [1536], replicated
- output 2: float32 [65536], P('dp')
All inputs are finite; a program needn't handle non-finite values.
Results may differ from the reference program's by a relative error of at most 0.001.
Values sent between devices are 32-bit elements.
A program may use at most 1 GiB of HBM per device.

```python
import jax
import jax.numpy as jnp
from jax import lax

FEATURES = 1536
ROWS_DEV = 8192
GROUPS = 8
LOW_RANK = 128

TOTAL_ROWS = ROWS_DEV * GROUPS
HIGHEST = lax.Precision.HIGHEST
CONTRACT_ROWS = (((0,), (0,)), ((), ()))


def setup_inputs(seed: int = 0) -> dict:
    keys = jax.random.split(jax.random.key(seed), 9)
    col_scale = jnp.exp(jax.random.uniform(keys[0], (FEATURES,), jnp.float32, -3.0, 0.0))
    base = jax.random.normal(keys[1], (TOTAL_ROWS, FEATURES), jnp.float32)
    factors = jax.random.normal(keys[2], (TOTAL_ROWS, LOW_RANK), jnp.float32)
    mixing = jax.random.normal(keys[3], (FEATURES, LOW_RANK), jnp.float32) * (0.5 * LOW_RANK ** -0.5)
    shard_gain = jnp.exp(jax.random.uniform(keys[4], (GROUPS, 1), jnp.float32, -1.0, 1.0))
    row_jitter = jnp.exp(jax.random.uniform(keys[5], (GROUPS, ROWS_DEV), jnp.float32, -0.25, 0.25))
    row_gain = (shard_gain * row_jitter).reshape(TOTAL_ROWS, 1)
    mixed = jnp.dot(factors, mixing.T, precision=HIGHEST)
    design = (base * col_scale + mixed) * (row_gain * FEATURES ** -0.5)
    x_true = jax.random.normal(keys[6], (FEATURES,), jnp.float32)
    noise = 0.3 * jax.random.normal(keys[7], (TOTAL_ROWS,), jnp.float32) * row_gain[:, 0]
    target = jnp.dot(design, x_true, precision=HIGHEST) + noise
    diag_mean = jnp.sum(design * design) / FEATURES
    ridge = diag_mean * jax.random.uniform(keys[8], (), jnp.float32, 0.01, 0.04)
    return {'design': design, 'target': target, 'ridge': ridge}


def reference(design, target, ridge):
    gram_mat = lax.dot_general(design, design, CONTRACT_ROWS, precision=HIGHEST, preferred_element_type=jnp.float32)
    moment_vec = lax.dot_general(design, target, CONTRACT_ROWS, precision=HIGHEST, preferred_element_type=jnp.float32)
    chol_low = jnp.linalg.cholesky(gram_mat + ridge * jnp.eye(FEATURES, dtype=jnp.float32))
    half_solve = lax.linalg.triangular_solve(chol_low, moment_vec[:, None], left_side=True, lower=True)
    coeffs = lax.linalg.triangular_solve(chol_low, half_solve, left_side=True, lower=True, transpose_a=True)[:, 0]
    residual = target - jnp.dot(design, coeffs, precision=HIGHEST, preferred_element_type=jnp.float32)
    return coeffs, residual
```

```python
import functools
import jax, jax.numpy as jnp
from jax import lax
from jax.experimental import pallas as pl
from jax.experimental.pallas import tpu as pltpu
from jax.sharding import PartitionSpec as P

HIGHEST = lax.Precision.HIGHEST
F32 = jnp.float32
SUB, HALF, PANEL = 16, 128, 256


def dot(a, b, dims=((1,), (0,))):
    return lax.dot_general(a, b, (dims, ((), ())), precision=HIGHEST, preferred_element_type=F32)


def micro_rows(left, right, col0):
    rows = lax.broadcasted_iota(jnp.int32, (SUB, HALF), 0)
    cols = [jnp.broadcast_to(left[:, col0 + c:col0 + c + 1], (SUB, HALF)) for c in range(SUB)]
    pivots = cols[0]
    for p in range(SUB):
        inv = 1.0 / cols[p][p:p + 1, :]
        fac = jnp.where(rows > p, cols[p] * inv, 0.0)
        for c in range(p + 1, SUB):
            cols[c] = cols[c] - fac * cols[c][p:p + 1, :]
        left = left - fac * left[p:p + 1, :]
        right = right - fac * right[p:p + 1, :]
        pivots = jnp.where(rows == p, cols[p], pivots)
    scale = lax.rsqrt(pivots)
    return left * scale, right * scale


def invert_factor(work, inv_ref, row0):
    for m in range(HALF // SUB):
        r = m * SUB
        left, right = micro_rows(work[r:r + SUB, :HALF], work[r:r + SUB, HALF:], r)
        inv_ref[row0 + r:row0 + r + SUB, row0:row0 + HALF] = right
        if r + SUB < HALF:
            both = jnp.concatenate([left, right], axis=1)
            upd = dot(left, both, ((0,), (0,)))
            work[r + SUB:, :] = work[r + SUB:, :] - upd[r + SUB:, :]


def eye(n):
    return jnp.where(lax.broadcasted_iota(jnp.int32, (n, n), 0) == lax.broadcasted_iota(jnp.int32, (n, n), 1), 1.0, 0.0).astype(F32)


def factor(up, inv, work, n, width):
    panels = n // PANEL

    def step(k, _):
        r0 = pl.multiple_of(k * PANEL, PANEL)
        winv = inv.at[k]
        winv[...] = jnp.zeros((PANEL, PANEL), F32)
        work[:, :HALF] = up[pl.ds(r0, HALF), pl.ds(r0, HALF)]
        work[:, HALF:] = eye(HALF)
        invert_factor(work, winv, 0)
        w1 = winv[:HALF, :HALF]
        u12 = dot(w1, up[pl.ds(r0, HALF), pl.ds(r0 + HALF, HALF)])
        work[:, :HALF] = up[pl.ds(r0 + HALF, HALF), pl.ds(r0 + HALF, HALF)] - dot(u12, u12, ((0,), (0,)))
        work[:, HALF:] = eye(HALF)
        t = dot(u12, w1, ((0,), (0,)))
        invert_factor(work, winv, HALF)
        w2 = winv[HALF:, HALF:]
        winv[HALF:, :HALF] = -dot(w2, t)
        for kk in range(panels):
            @pl.when(k == kk)
            def _():
                a, b = kk * PANEL, (kk + 1) * PANEL
                up[a:b, b:] = dot(winv[...], up[a:b, b:])
                for i in range(kk + 1, panels):
                    c = i * PANEL
                    up[c:c + PANEL, c:] = up[c:c + PANEL, c:] - dot(up[a:b, c:c + PANEL], up[a:b, c:], ((0,), (0,)))
        return 0

    lax.fori_loop(0, panels, step, 0)


def back_solve(up, inv, x_ref, n, rhs_col):
    panels = n // PANEL
    for k in range(panels - 1, -1, -1):
        a, b = k * PANEL, (k + 1) * PANEL
        v = up[a:b, rhs_col:rhs_col + 1]
        if b < n:
            v = v - jnp.sum(up[a:b, b:n] * x_ref[0:1, b:n], axis=1, keepdims=True)
        x_ref[0:1, a:b] = jnp.sum(inv[k] * v, axis=0, keepdims=True)


def solve_kernel(n, gram, x_ref, up, inv, work, sem):
    copy = pltpu.make_async_copy(gram, up, sem)
    copy.start()
    copy.wait()
    factor(up, inv, work, n, up.shape[1])
    back_solve(up, inv, x_ref, n, n)


def solve(gram_aug):
    n, width = gram_aug.shape
    return pl.pallas_call(
        functools.partial(solve_kernel, n),
        out_shape=jax.ShapeDtypeStruct((1, n), F32),
        in_specs=[pl.BlockSpec(memory_space=pl.ANY)],
        out_specs=pl.BlockSpec(memory_space=pltpu.VMEM),
        scratch_shapes=[
            pltpu.VMEM((n, width), F32),
            pltpu.VMEM((n // PANEL, PANEL, PANEL), F32),
            pltpu.VMEM((HALF, 2 * HALF), F32),
            pltpu.SemaphoreType.DMA,
        ],
        compiler_params=pltpu.CompilerParams(vmem_limit_bytes=48 * 1024 * 1024),
        cost_estimate=pl.CostEstimate(flops=int(n) ** 3 * 4, bytes_accessed=4 * n * width, transcendentals=0),
        name="factor_solve",
    )(gram_aug)


def solution(mesh):
    col_ways = mesh.shape['tp']

    def local_fit(design_blk, target_blk, ridge):
        rows_dev, cols_dev = design_blk.shape
        features = cols_dev * col_ways
        sub_rows = rows_dev // col_ways
        col_index = lax.axis_index('tp')
        row_panel = lax.all_to_all(design_blk, 'tp', 0, 1, tiled=True)
        target_part = lax.dynamic_slice_in_dim(target_blk, col_index * sub_rows, sub_rows)
        target_pad = jnp.pad(target_part[:, None], ((0, 0), (0, HALF - 1)))
        gram_part = dot(row_panel, jnp.concatenate([row_panel, target_pad], axis=1), ((0,), (0,)))
        gram_aug = lax.psum(gram_part, ('tp', 'dp'))
        row_id = lax.broadcasted_iota(jnp.int32, gram_aug.shape, 0)
        col_id = lax.broadcasted_iota(jnp.int32, gram_aug.shape, 1)
        coeffs = solve(jnp.where(row_id == col_id, gram_aug + ridge, gram_aug))[0]
        coeff_blk = lax.dynamic_slice_in_dim(coeffs, col_index * cols_dev, cols_dev)
        fitted = lax.psum(dot(design_blk, coeff_blk, ((1,), (0,))), 'tp')
        return coeffs, target_blk - fitted

    return jax.shard_map(local_fit, mesh=mesh, in_specs=(P('dp', 'tp'), P('dp'), P()), out_specs=(P(), P('dp')), check_vma=False)
```

```python
import functools
import jax
import jax.numpy as jnp
from jax import lax
from jax.experimental import pallas as pl
from jax.experimental.pallas import tpu as pltpu
from jax.sharding import PartitionSpec as P

HIGHEST = lax.Precision.HIGHEST
F32 = jnp.float32
SUB, HALF, PANEL, BLOCK, EXTRA = 16, 128, 256, 384, 128
PAIR = 2 * BLOCK
MESH = pl.DeviceIdType.MESH
MIB = 1024 * 1024


def dot(a, b, dims=((1,), (0,))):
    return lax.dot_general(a, b, (dims, ((), ())), precision=HIGHEST, preferred_element_type=F32)


def micro_rows(left, right, col0):
    rows = lax.broadcasted_iota(jnp.int32, (SUB, HALF), 0)
    cols = [jnp.broadcast_to(left[:, col0 + c:col0 + c + 1], (SUB, HALF)) for c in range(SUB)]
    pivots = cols[0]
    for p in range(SUB):
        inv = 1.0 / cols[p][p:p + 1, :]
        fac = jnp.where(rows > p, cols[p] * inv, 0.0)
        for c in range(p + 1, SUB):
            cols[c] = cols[c] - fac * cols[c][p:p + 1, :]
        left = left - fac * left[p:p + 1, :]
        right = right - fac * right[p:p + 1, :]
        pivots = jnp.where(rows == p, cols[p], pivots)
    scale = lax.rsqrt(pivots)
    return left * scale, right * scale


def invert_factor(work, inv_ref, row0):
    for m in range(HALF // SUB):
        r = m * SUB
        left, right = micro_rows(work[r:r + SUB, :HALF], work[r:r + SUB, HALF:], r)
        inv_ref[row0 + r:row0 + r + SUB, row0:row0 + HALF] = right
        if r + SUB < HALF:
            both = jnp.concatenate([left, right], axis=1)
            upd = dot(left, both, ((0,), (0,)))
            work[r + SUB:, :] = work[r + SUB:, :] - upd[r + SUB:, :]


def eye(n):
    return jnp.where(lax.broadcasted_iota(jnp.int32, (n, n), 0) == lax.broadcasted_iota(jnp.int32, (n, n), 1), 1.0, 0.0).astype(F32)


def factor(up, inv, work, n):
    panels = n // PANEL

    def step(k, _):
        r0 = pl.multiple_of(k * PANEL, PANEL)
        winv = inv.at[k]
        winv[...] = jnp.zeros((PANEL, PANEL), F32)
        work[:, :HALF] = up[pl.ds(r0, HALF), pl.ds(r0, HALF)]
        work[:, HALF:] = eye(HALF)
        invert_factor(work, winv, 0)
        w1 = winv[:HALF, :HALF]
        u12 = dot(w1, up[pl.ds(r0, HALF), pl.ds(r0 + HALF, HALF)])
        work[:, :HALF] = up[pl.ds(r0 + HALF, HALF), pl.ds(r0 + HALF, HALF)] - dot(u12, u12, ((0,), (0,)))
        work[:, HALF:] = eye(HALF)
        t = dot(u12, w1, ((0,), (0,)))
        invert_factor(work, winv, HALF)
        w2 = winv[HALF:, HALF:]
        winv[HALF:, :HALF] = -dot(w2, t)
        for kk in range(panels):
            @pl.when(k == kk)
            def _():
                a, b = kk * PANEL, (kk + 1) * PANEL
                up[a:b, b:] = dot(winv[...], up[a:b, b:])
                for i in range(kk + 1, panels):
                    c = i * PANEL
                    up[c:c + PANEL, c:] = up[c:c + PANEL, c:] - dot(up[a:b, c:c + PANEL], up[a:b, c:], ((0,), (0,)))
        return 0

    lax.fori_loop(0, panels, step, 0)


def places():
    z, dp = lax.axis_index('tp'), lax.axis_index('dp')
    core, x, y = lax.rem(dp, 2), lax.rem(dp // 2, 2), dp // 4
    return z, dp, core, x, y


def z_peers(z):
    return (z + 1 - 2 * lax.rem(z, 2), z + 2 - 4 * (z // 2), 3 - z)


def reduce_kernel(rows, gather, part, out, acc, full, got_core, got_a, got_b, got_a2, got_b2, got_z, send_sem, recv_sem, out_sem):
    z, dp, core, x, y = places()
    half, quart, eighth, sixt = rows // 2, rows // 4, rows // 8, rows // 16
    core_peer = {'tp': z, 'dp': dp + 1 - 2 * core}
    x_peer = {'tp': z, 'dp': dp + 2 - 4 * x}
    y_peer = {'tp': z, 'dp': dp + 4 - 8 * y}
    z_peer = [{'tp': p, 'dp': dp} for p in z_peers(z)]
    peers = [core_peer, x_peer, y_peer] + z_peer
    barrier = pltpu.get_barrier_semaphore()
    for peer in peers:
        pl.semaphore_signal(barrier, inc=1, device_id=peer, device_id_type=MESH)
    pl.semaphore_wait(barrier, len(peers))
    count = [0]

    def start(src, dst, peer):
        i = count[0]
        count[0] += 1
        copy = pltpu.make_async_remote_copy(src_ref=src, dst_ref=dst, send_sem=send_sem.at[i], recv_sem=recv_sem.at[i], device_id=peer, device_id_type=MESH)
        copy.start()
        return copy

    def at(base, size):
        return pl.ds(pl.multiple_of(base, 8), size)

    own = core * half
    copy = start(part.at[at((1 - core) * half, half)], got_core, core_peer)
    copy.wait()
    acc[...] = part[at(own, half)] + got_core[...]
    copies = [start(acc.at[at((1 - x) * eighth, eighth)], got_a, x_peer), start(acc.at[at(quart + (1 - y) * eighth, eighth)], got_b, y_peer)]
    a1, b1 = x * eighth, quart + y * eighth
    copies[0].wait()
    acc[at(a1, eighth)] = acc[at(a1, eighth)] + got_a[...]
    copies[1].wait()
    acc[at(b1, eighth)] = acc[at(b1, eighth)] + got_b[...]
    copies = [start(acc.at[at(a1 + (1 - y) * sixt, sixt)], got_a2, y_peer), start(acc.at[at(b1 + (1 - x) * sixt, sixt)], got_b2, x_peer)]
    a2, b2 = a1 + y * sixt, b1 + x * sixt
    if gather:
        copies[0].wait()
        full[z, at(own + a2, sixt)] = acc[at(a2, sixt)] + got_a2[...]
        copies[1].wait()
        full[z, at(own + b2, sixt)] = acc[at(b2, sixt)] + got_b2[...]
        copies = []
        for piece in (a2, b2):
            ref = full.at[z, at(own + piece, sixt)]
            copies += [start(ref, ref, peer) for peer in z_peer]
        for copy in copies:
            copy.wait()
    else:
        copies[0].wait()
        acc[at(a2, sixt)] = acc[at(a2, sixt)] + got_a2[...]
        copies[1].wait()
        acc[at(b2, sixt)] = acc[at(b2, sixt)] + got_b2[...]
        share = sixt // 4
        copies = []
        for k, piece in enumerate((a2, b2)):
            for j, peer in enumerate(z_peer):
                copies.append(start(acc.at[at(piece + peer['tp'] * share, share)], got_z.at[2 * j + k], peer))
        for copy in copies:
            copy.wait()
        copies = []
        for k, piece in enumerate((a2, b2)):
            mine = piece + z * share
            full[0, at(own + mine, share)] = (acc[at(mine, share)] + got_z[k]) + (got_z[2 + k] + got_z[4 + k])
            ref = full.at[0, at(own + mine, share)]
            copies += [start(ref, ref, peer) for peer in z_peer]
        for copy in copies:
            copy.wait()
    for sizes in (((a2, sixt, y_peer), (b2, sixt, x_peer)), ((a1, eighth, x_peer), (b1, eighth, y_peer)), ((0, half, core_peer),)):
        copies = []
        for base, size, peer in sizes:
            ref = full.at[:, at(own + base, size)]
            copies.append(start(ref, ref, peer))
        for copy in copies:
            copy.wait()
    copy = pltpu.make_async_copy(full, out, out_sem)
    copy.start()
    copy.wait()


def reduce_all(part, gather, ident):
    rows = part.shape[0]
    slabs = 4 if gather else 1
    n = 1 + 2 + 2 + 6 + (0 if gather else 6) + 2 + 2 + 1
    return pl.pallas_call(
        functools.partial(reduce_kernel, rows, gather),
        out_shape=jax.ShapeDtypeStruct((slabs, rows, BLOCK), F32),
        in_specs=[pl.BlockSpec(memory_space=pltpu.VMEM)],
        out_specs=pl.BlockSpec(memory_space=pl.ANY),
        scratch_shapes=[
            pltpu.VMEM((rows // 2, BLOCK), F32),
            pltpu.VMEM((slabs, rows, BLOCK), F32),
            pltpu.VMEM((rows // 2, BLOCK), F32),
            pltpu.VMEM((rows // 8, BLOCK), F32),
            pltpu.VMEM((rows // 8, BLOCK), F32),
            pltpu.VMEM((rows // 16, BLOCK), F32),
            pltpu.VMEM((rows // 16, BLOCK), F32),
            pltpu.VMEM((6, 8 if gather else rows // 64, BLOCK), F32),
            pltpu.SemaphoreType.DMA((n,)),
            pltpu.SemaphoreType.DMA((n,)),
            pltpu.SemaphoreType.DMA,
        ],
        compiler_params=pltpu.CompilerParams(collective_id=ident, has_side_effects=True, vmem_limit_bytes=30 * 1024 * 1024),
        cost_estimate=pl.CostEstimate(flops=rows * 2000, bytes_accessed=100_000_000, transcendentals=0),
        name="reduce_gather" if gather else "reduce_all",
    )(part)


def lower_back(up, inv, x_ref, x0, base):
    for k in range(PAIR // PANEL - 1, -1, -1):
        a, b = k * PANEL, (k + 1) * PANEL
        v = base(a, b)
        if b < PAIR:
            v = v - jnp.sum(up[a:b, b:PAIR] * x_ref[0:1, x0 + b:x0 + PAIR], axis=1, keepdims=True)
        x_ref[0:1, x0 + a:x0 + b] = jnp.sum(inv[k] * v, axis=0, keepdims=True)


def load_half(planes, stage, sems, first, up, ridge):
    copies = [pltpu.make_async_copy(planes.at[first + i], stage.at[i], sems.at[i]) for i in range(2)]
    for copy in copies:
        copy.start()
    for copy in copies:
        copy.wait()
    diag = eye(BLOCK) * ridge
    for i in range(2):
        a, b = i * BLOCK, (i + 1) * BLOCK
        up[a:b, a:b] = stage[i, :BLOCK] + diag
        up[a:b, PAIR:] = stage[i, PAIR:].T
    up[:BLOCK, BLOCK:PAIR] = stage[0, BLOCK:PAIR] + stage[1, BLOCK:PAIR]


def low_kernel(planes, ridge, up, inv, stage, work, sems):
    load_half(planes, stage, sems, 0, up, ridge[0, 0])
    factor(up, inv, work, PAIR)


def high_kernel(planes, ridge, up_low, inv_low, cross, x_ref, stage, mid, up, inv, work, sems):
    load_half(planes, stage, sems, 2, up, ridge[0, 0])
    for i in range(2):
        for j in range(2):
            r = (2 * i + j) * BLOCK
            mid[i * BLOCK:(i + 1) * BLOCK, j * BLOCK:(j + 1) * BLOCK] = cross[0, r:r + BLOCK, :]
    mid[:, PAIR:] = up_low[:, PAIR:]
    panels = PAIR // PANEL
    for k in range(panels):
        a, b = k * PANEL, (k + 1) * PANEL
        mid[a:b, :PAIR] = dot(inv_low[k], mid[a:b, :PAIR])
        for i in range(k + 1, panels):
            c = i * PANEL
            mid[c:c + PANEL, :PAIR] = mid[c:c + PANEL, :PAIR] - dot(up_low[a:b, c:c + PANEL], mid[a:b, :PAIR], ((0,), (0,)))
    for i in range(panels):
        c = i * PANEL
        up[c:c + PANEL, c:] = up[c:c + PANEL, c:] - dot(mid[:, c:c + PANEL], mid[:, c:], ((0,), (0,)))
    factor(up, inv, work, PAIR)
    lower_back(up, inv, x_ref, PAIR, lambda a, b: up[a:b, PAIR:PAIR + 1])
    lower_back(up_low, inv_low, x_ref, 0, lambda a, b: up_low[a:b, PAIR:PAIR + 1] - jnp.sum(
        mid[a:b, :PAIR] * x_ref[0:1, PAIR:], axis=1, keepdims=True))


VM = pl.BlockSpec(memory_space=pltpu.VMEM)
SM = pl.BlockSpec(memory_space=pltpu.SMEM)
HB = pl.BlockSpec(memory_space=pl.ANY)
PANELS_SHAPE = (PAIR // PANEL, PANEL, PANEL)


def factor_low(planes, ridge):
    rows = planes.shape[1]
    return pl.pallas_call(
        low_kernel,
        out_shape=(jax.ShapeDtypeStruct((PAIR, PAIR + EXTRA), F32), jax.ShapeDtypeStruct(PANELS_SHAPE, F32)),
        in_specs=[HB, SM],
        out_specs=(VM, VM),
        scratch_shapes=[pltpu.VMEM((2, rows, BLOCK), F32), pltpu.VMEM((HALF, 2 * HALF), F32), pltpu.SemaphoreType.DMA((2,))],
        compiler_params=pltpu.CompilerParams(vmem_limit_bytes=24 * MIB),
        cost_estimate=pl.CostEstimate(flops=40_000_000_000, bytes_accessed=10_000_000, transcendentals=0),
        name="factor_low",
    )(planes, ridge)


def factor_high(planes, ridge, up_low, inv_low, cross):
    rows = planes.shape[1]
    return pl.pallas_call(
        high_kernel,
        out_shape=jax.ShapeDtypeStruct((1, 2 * PAIR), F32),
        in_specs=[HB, SM, VM, VM, VM],
        out_specs=VM,
        scratch_shapes=[
            pltpu.VMEM((2, rows, BLOCK), F32),
            pltpu.VMEM((PAIR, PAIR + EXTRA), F32),
            pltpu.VMEM((PAIR, PAIR + EXTRA), F32),
            pltpu.VMEM(PANELS_SHAPE, F32),
            pltpu.VMEM((HALF, 2 * HALF), F32),
            pltpu.SemaphoreType.DMA((2,)),
        ],
        compiler_params=pltpu.CompilerParams(vmem_limit_bytes=32 * MIB),
        cost_estimate=pl.CostEstimate(flops=50_000_000_000, bytes_accessed=10_000_000, transcendentals=0),
        name="factor_high",
    )(planes, ridge, up_low, inv_low, cross)


def cross_kernel(slot, steps, own, mate, far, prev, out, near, total):
    z = lax.axis_index('tp')
    i = pl.program_id(0)
    odd = lax.rem(z, 2)
    near[:, pl.ds(pl.multiple_of(odd * BLOCK, BLOCK), BLOCK)] = own[...]
    near[:, pl.ds(pl.multiple_of((1 - odd) * BLOCK, BLOCK), BLOCK)] = mate[...]

    @pl.when(i == 0)
    def _():
        total[...] = jnp.zeros_like(total)

    @pl.when(z < 2)
    def _():
        total[...] += dot(near[...], far[...], ((0,), (0,)))

    @pl.when(z >= 2)
    def _():
        total[:BLOCK] += dot(far[...], near[:, :BLOCK], ((0,), (0,)))
        total[BLOCK:] += dot(far[...], near[:, BLOCK:], ((0,), (0,)))

    def place(src, far_odd):
        for n in range(2):
            r = jnp.where(z < 2, 2 * n + far_odd, 2 * far_odd + n) * BLOCK
            out[pl.ds(pl.multiple_of(r, BLOCK), BLOCK), :] = src[n * BLOCK:(n + 1) * BLOCK, :]

    @pl.when(i == steps - 1)
    def _():
        if slot == 0:
            out[...] = total[...]
        else:
            place(prev, 1 - odd)
            place(total, odd)


def cross_gram(slot, design_blk, mate, far, prev, z_row):
    quarter = mate.shape[0]
    tile = 512
    steps = quarter // tile
    tile_spec = pl.BlockSpec((tile, BLOCK), lambda i, zr: (i, 0))
    whole = pl.BlockSpec(prev.shape, lambda i, zr: (0, 0))
    out_rows = PAIR if slot == 0 else 2 * PAIR
    return pl.pallas_call(
        lambda zr, *refs: cross_kernel(slot, steps, *refs),
        out_shape=jax.ShapeDtypeStruct((out_rows, BLOCK), F32),
        grid_spec=pltpu.PrefetchScalarGridSpec(
            num_scalar_prefetch=1,
            grid=(steps,),
            in_specs=[pl.BlockSpec((tile, BLOCK), lambda i, zr: (zr[0] * steps + i, 0)), tile_spec, tile_spec, whole],
            out_specs=pl.BlockSpec((out_rows, BLOCK), lambda i, zr: (0, 0)),
            scratch_shapes=[pltpu.VMEM((tile, PAIR), F32), pltpu.VMEM((PAIR, BLOCK), F32)],
        ),
        compiler_params=pltpu.CompilerParams(dimension_semantics=("arbitrary",), vmem_limit_bytes=30 * MIB),
        cost_estimate=pl.CostEstimate(flops=8_000_000_000, bytes_accessed=12_000_000, transcendentals=0),
    )(z_row, design_blk, mate, far, prev)


def residual_kernel(steps, design, x_ref, target, out, fits, send_sem, recv_sem):
    z, dp = lax.axis_index('tp'), lax.axis_index('dp')
    i = pl.program_id(0)
    tile = design.shape[0]
    peers = [{'tp': p, 'dp': dp} for p in z_peers(z)]

    @pl.when(i == 0)
    def _():
        barrier = pltpu.get_barrier_semaphore()
        for peer in peers:
            pl.semaphore_signal(barrier, inc=1, device_id=peer, device_id_type=MESH)
        pl.semaphore_wait(barrier, 3)

    x = [x_ref[0:1, pl.ds(pl.multiple_of(z * BLOCK + c * HALF, HALF), HALF)] for c in range(BLOCK // HALF)]
    rows = []
    for r in range(tile // HALF):
        t = sum(design[r * HALF:(r + 1) * HALF, c * HALF:(c + 1) * HALF] * x[c] for c in range(BLOCK // HALF))
        rows.append(jnp.sum(t.T, axis=0, keepdims=True))
    per = tile // HALF
    fits[0, pl.ds(pl.multiple_of(i * per, per), per), :] = jnp.concatenate(rows, axis=0)

    @pl.when(i == steps - 1)
    def _():
        copies = []
        for j, peer in enumerate(peers):
            copy = pltpu.make_async_remote_copy(src_ref=fits.at[0], dst_ref=fits.at[j + 1], send_sem=send_sem.at[j], recv_sem=recv_sem.at[j], device_id=peer, device_id_type=MESH)
            copy.start()
            copies.append(copy)
        for copy in copies:
            copy.wait()
        lo = jnp.where(z % 2 == 0, fits[0] + fits[1], fits[1] + fits[0])
        hi = jnp.where(z % 2 == 0, fits[2] + fits[3], fits[3] + fits[2])
        out[...] = target[...] - (lo + hi)


def residual(design_blk, x_row, target_tile):
    rows = design_blk.shape[0]
    tile = 1024
    steps = rows // tile
    whole = pl.BlockSpec(target_tile.shape, lambda i: (0, 0))
    return pl.pallas_call(
        functools.partial(residual_kernel, steps),
        out_shape=jax.ShapeDtypeStruct(target_tile.shape, F32),
        grid=(steps,),
        in_specs=[pl.BlockSpec((tile, BLOCK), lambda i: (i, 0)), pl.BlockSpec(x_row.shape, lambda i: (0, 0)), whole],
        out_specs=whole,
        scratch_shapes=[pltpu.VMEM((4,) + target_tile.shape, F32), pltpu.SemaphoreType.DMA((3,)), pltpu.SemaphoreType.DMA((3,))],
        compiler_params=pltpu.CompilerParams(collective_id=3, has_side_effects=True, dimension_semantics=("arbitrary",), vmem_limit_bytes=24 * MIB),
        cost_estimate=pl.CostEstimate(flops=6_000_000_000, bytes_accessed=13_000_000, transcendentals=0),
        name="residual",
    )(design_blk, x_row, target_tile)


def solution(mesh):
    col_ways, row_ways = mesh.shape['tp'], mesh.shape['dp']

    def swap(block, mask):
        pairs = [(t * row_ways + d, (t ^ mask) * row_ways + d) for t in range(col_ways) for d in range(row_ways)]
        return lax.ppermute(block, ('tp', 'dp'), pairs)

    def local_fit(design_blk, target_blk, ridge):
        rows_dev, _ = design_blk.shape
        quarter_rows = rows_dev // col_ways
        z = lax.axis_index('tp')

        def quarter(index):
            return lax.dynamic_slice_in_dim(design_blk, index * quarter_rows, quarter_rows)

        mate_a = swap(quarter(z ^ 1), 1)
        mate_b = swap(quarter(z ^ 3), 1)
        far_c = swap(quarter(z ^ 3), 3)
        far_d = swap(quarter(z ^ 2), 2)
        own_gram = dot(design_blk, design_blk, ((0,), (0,)))
        moment = dot(target_blk[None, :], design_blk)
        pair_gram = dot(quarter(z), mate_a, ((0,), (0,))) + dot(quarter(z ^ 2), mate_b, ((0,), (0,)))
        pair_gram = jnp.where(z % 2 == 0, pair_gram, pair_gram.T)
        part = jnp.concatenate([own_gram, pair_gram, jnp.pad(moment, ((0, EXTRA - 1), (0, 0)))], axis=0)
        planes = reduce_all(part, True, 1)
        ridge_cell = jnp.reshape(ridge, (1, 1))
        up_low, inv_low = factor_low(planes, ridge_cell)
        z_row = jnp.reshape(z, (1,)).astype(jnp.int32)
        first = cross_gram(0, design_blk, mate_a, far_c, jnp.zeros((8, HALF), F32), z_row)
        cross = cross_gram(1, design_blk, mate_a, far_d, first, z_row)
        cross = reduce_all(cross, False, 2)
        x_row = factor_high(planes, ridge_cell, up_low, inv_low, cross)
        left = residual(design_blk, x_row, jnp.reshape(target_blk, (rows_dev // HALF, HALF)))
        return x_row[0], jnp.reshape(left, (rows_dev,))

    return jax.shard_map(local_fit, mesh=mesh, in_specs=(P('dp', 'tp'), P('dp'), P()), out_specs=(P(), P('dp')), check_vma=False)
```

```python
import functools
import jax
import jax.numpy as jnp
from jax import lax
from jax.experimental import pallas as pl
from jax.experimental.pallas import tpu as pltpu
from jax.sharding import PartitionSpec as P

HIGHEST = lax.Precision.HIGHEST
F32 = jnp.float32
SUB, HALF, PANEL, BLOCK, EXTRA = 16, 128, 256, 384, 128
PAIR = 2 * BLOCK
MESH = pl.DeviceIdType.MESH
MIB = 1024 * 1024


def dot(a, b, dims=((1,), (0,))):
    return lax.dot_general(a, b, (dims, ((), ())), precision=HIGHEST, preferred_element_type=F32)


def micro_rows(left, right, col0):
    rows = lax.broadcasted_iota(jnp.int32, (SUB, HALF), 0)
    cols = [jnp.broadcast_to(left[:, col0 + c:col0 + c + 1], (SUB, HALF)) for c in range(SUB)]
    pivots = cols[0]
    for p in range(SUB):
        inv = 1.0 / cols[p][p:p + 1, :]
        fac = jnp.where(rows > p, cols[p] * inv, 0.0)
        for c in range(p + 1, SUB):
            cols[c] = cols[c] - fac * cols[c][p:p + 1, :]
        left = left - fac * left[p:p + 1, :]
        right = right - fac * right[p:p + 1, :]
        pivots = jnp.where(rows == p, cols[p], pivots)
    scale = lax.rsqrt(pivots)
    return left * scale, right * scale


def invert_factor(work, inv_ref):
    for m in range(HALF // SUB):
        r = m * SUB
        left, right = micro_rows(work[r:r + SUB, :HALF], work[r:r + SUB, HALF:], r)
        inv_ref[r:r + SUB, :] = right
        if r + SUB < HALF:
            both = jnp.concatenate([left, right], axis=1)
            upd = dot(left, both, ((0,), (0,)))
            work[r + SUB:, :] = work[r + SUB:, :] - upd[r + SUB:, :]


def eye(n):
    rows = lax.broadcasted_iota(jnp.int32, (n, n), 0)
    return jnp.where(rows == lax.broadcasted_iota(jnp.int32, (n, n), 1), 1.0, 0.0).astype(F32)


def factor(up, inv, work, small, n):
    panels = n // PANEL
    first, carry = small.at[0], small.at[1]

    def step(t, _):
        k, odd = t // 2, lax.rem(t, 2)
        r0 = pl.multiple_of(t * HALF, HALF)
        r1 = pl.multiple_of(t * HALF + HALF * (1 - odd), HALF)
        work[:, :HALF] = up[pl.ds(r0, HALF), pl.ds(r0, HALF)]
        work[:, HALF:] = eye(HALF)
        invert_factor(work, first)

        @pl.when(odd == 0)
        def _():
            w1 = first[...]
            inv[k] = jnp.zeros((PANEL, PANEL), F32)
            inv[k, :HALF, :HALF] = w1
            u12 = dot(w1, up[pl.ds(r0, HALF), pl.ds(r1, HALF)])
            both = dot(u12, jnp.concatenate([u12, w1], axis=1), ((0,), (0,)))
            up[pl.ds(r1, HALF), pl.ds(r1, HALF)] = up[pl.ds(r1, HALF), pl.ds(r1, HALF)] - both[:, :HALF]
            carry[...] = both[:, HALF:]

        @pl.when(odd == 1)
        def _():
            w2 = first[...]
            inv[k, HALF:, HALF:] = w2
            inv[k, HALF:, :HALF] = -dot(w2, carry[...])

        for kk in range(panels):
            @pl.when(t == 2 * kk + 1)
            def _():
                a, b = kk * PANEL, (kk + 1) * PANEL
                up[a:b, b:] = dot(inv[kk], up[a:b, b:])
                for i in range(kk + 1, panels):
                    c = i * PANEL
                    up[c:c + PANEL, c:] = up[c:c + PANEL, c:] - dot(up[a:b, c:c + PANEL], up[a:b, c:], ((0,), (0,)))
        return 0

    lax.fori_loop(0, 2 * panels, step, 0)


def places():
    z, dp = lax.axis_index('tp'), lax.axis_index('dp')
    core, x, y = lax.rem(dp, 2), lax.rem(dp // 2, 2), dp // 4
    return z, dp, core, x, y


def z_peers(z):
    return (z + 1 - 2 * lax.rem(z, 2), z + 2 - 4 * (z // 2), 3 - z)


def plane_peers(z, dp, core, x, y):
    return ({'tp': z, 'dp': dp + 1 - 2 * core}, {'tp': z, 'dp': dp + 2 - 4 * x}, {'tp': z, 'dp': dp + 4 - 8 * y})


def meet(peers):
    barrier = pltpu.get_barrier_semaphore()
    for peer in peers:
        pl.semaphore_signal(barrier, inc=1, device_id=peer, device_id_type=MESH)
    pl.semaphore_wait(barrier, len(peers))


def starter(send_sem, recv_sem):
    count = [0]

    def start(src, dst, peer):
        i = count[0]
        count[0] += 1
        copy = pltpu.make_async_remote_copy(src_ref=src, dst_ref=dst, send_sem=send_sem.at[i], recv_sem=recv_sem.at[i], device_id=peer, device_id_type=MESH)
        copy.start()
        return copy

    return start


def at(base, size):
    return pl.ds(pl.multiple_of(base, 8), size)


def spans(rows, core, x, y):
    half, quart, eighth, sixt = rows // 2, rows // 4, rows // 8, rows // 16
    a1, b1 = x * eighth, quart + y * eighth
    return core * half, a1, b1, a1 + y * sixt, b1 + x * sixt


def plane_scatter(rows, part, acc, got, start, peers, where):
    _, _, core, x, y = where
    core_peer, x_peer, y_peer = peers
    half, quart, eighth, sixt = rows // 2, rows // 4, rows // 8, rows // 16
    own, a1, b1, a2, b2 = spans(rows, core, x, y)
    got_core, got_a, got_b, got_a2, got_b2 = got
    copy = start(part.at[at((1 - core) * half, half)], got_core, core_peer)
    yield
    copy.wait()
    acc[...] = part[at(own, half)] + got_core[...]
    copies = [start(acc.at[at((1 - x) * eighth, eighth)], got_a, x_peer), start(acc.at[at(quart + (1 - y) * eighth, eighth)], got_b, y_peer)]
    yield
    copies[0].wait()
    acc[at(a1, eighth)] = acc[at(a1, eighth)] + got_a[...]
    copies[1].wait()
    acc[at(b1, eighth)] = acc[at(b1, eighth)] + got_b[...]
    copies = [start(acc.at[at(a1 + (1 - y) * sixt, sixt)], got_a2, y_peer), start(acc.at[at(b1 + (1 - x) * sixt, sixt)], got_b2, x_peer)]
    yield
    copies[0].wait()
    acc[at(a2, sixt)] = acc[at(a2, sixt)] + got_a2[...]
    copies[1].wait()
    acc[at(b2, sixt)] = acc[at(b2, sixt)] + got_b2[...]


def plane_gather(rows, full, start, peers, where):
    _, _, core, x, y = where
    core_peer, x_peer, y_peer = peers
    half, eighth, sixt = rows // 2, rows // 8, rows // 16
    own, a1, b1, a2, b2 = spans(rows, core, x, y)
    for sizes in (((a2, sixt, y_peer), (b2, sixt, x_peer)), ((a1, eighth, x_peer), (b1, eighth, y_peer)), ((0, half, core_peer),)):
        copies = []
        for base, size, peer in sizes:
            ref = full.at[:, at(own + base, size)]
            copies.append(start(ref, ref, peer))
        yield
        for copy in copies:
            copy.wait()


def in_turn(chunks):
    chunks = list(chunks)
    while chunks:
        chunks = [chunk for chunk in chunks if next(chunk, chunks) is not chunks]


def wait_all(copies):
    for copy in copies:
        copy.wait()


def sum_chunk(rows, part, acc, full, got, got_z, start, peers, z_peer, where):
    z, _, core, x, y = where
    yield from plane_scatter(rows, part, acc, got, start, peers, where)
    own, _, _, a2, b2 = spans(rows, core, x, y)
    share = rows // 64
    copies = []
    for k, piece in enumerate((a2, b2)):
        for j, peer in enumerate(z_peer):
            copies.append(start(acc.at[at(piece + peer['tp'] * share, share)], got_z.at[2 * j + k], peer))
    yield
    wait_all(copies)
    copies = []
    for k, piece in enumerate((a2, b2)):
        mine = piece + z * share
        full[0, at(own + mine, share)] = (acc[at(mine, share)] + got_z[k]) + (got_z[2 + k] + got_z[4 + k])
        ref = full.at[0, at(own + mine, share)]
        copies += [start(ref, ref, peer) for peer in z_peer]
    yield
    wait_all(copies)
    yield from plane_gather(rows, full, start, peers, where)


CHUNKS = 2


def sum_kernel(rows, part, out, acc, full, g0, g1, g2, g3, g4, got_z, send_sem, recv_sem, out_sem):
    where = places()
    z, dp = where[:2]
    peers = plane_peers(*where)
    z_peer = [{'tp': p, 'dp': dp} for p in z_peers(z)]
    meet(list(peers) + z_peer)
    start = starter(send_sem, recv_sem)
    size = rows // CHUNKS
    in_turn(sum_chunk(size, part.at[c * size:(c + 1) * size], acc.at[c], full.at[:, c * size:(c + 1) * size],
                      [g.at[c] for g in (g0, g1, g2, g3, g4)], got_z.at[c], start, peers, z_peer, where) for c in range(CHUNKS))
    copy = pltpu.make_async_copy(full, out, out_sem)
    copy.start()
    copy.wait()


def stack_kernel(rows, part, out, acc, mine, g0, g1, g2, g3, g4, send_sem, recv_sem, out_sem):
    where = places()
    z, dp, core, x, y = where
    peers = plane_peers(*where)
    z_peer = [{'tp': p, 'dp': dp} for p in z_peers(z)]
    meet(list(peers) + z_peer)
    start = starter(send_sem, recv_sem)
    in_turn([plane_scatter(rows, part, acc.at[0], [g.at[0] for g in (g0, g1, g2, g3, g4)], start, peers, where)])
    _, _, _, a2, b2 = spans(rows, core, x, y)
    sixt = rows // 16
    mine[z, :sixt] = acc[0, at(a2, sixt)]
    mine[z, sixt:] = acc[0, at(b2, sixt)]
    wait_all([start(mine.at[z], mine.at[z], peer) for peer in z_peer])
    copy = pltpu.make_async_copy(mine, out, out_sem)
    copy.start()
    copy.wait()


def spread_kernel(rows, mine, out, full, send_sem, recv_sem, out_sem):
    where = places()
    _, _, core, x, y = where
    peers = plane_peers(*where)
    meet(peers)
    own, _, _, a2, b2 = spans(rows, core, x, y)
    sixt = rows // 16
    full[:, at(own + a2, sixt)] = mine[:, :sixt]
    full[:, at(own + b2, sixt)] = mine[:, sixt:]
    start = starter(send_sem, recv_sem)
    in_turn(plane_gather(rows, full.at[2 * c:2 * c + 2], start, peers, where) for c in range(2))
    copy = pltpu.make_async_copy(full, out, out_sem)
    copy.start()
    copy.wait()


def scatter_scratch(chunks, rows):
    return [pltpu.VMEM((chunks, rows // d, BLOCK), F32) for d in (2, 8, 8, 16, 16)]


def comm_call(body, rows, operand, out_shape, scratch, copies, ident):
    return pl.pallas_call(
        functools.partial(body, rows),
        out_shape=jax.ShapeDtypeStruct(out_shape, F32),
        in_specs=[pl.BlockSpec(memory_space=pltpu.VMEM)],
        out_specs=pl.BlockSpec(memory_space=pl.ANY),
        scratch_shapes=scratch + [pltpu.SemaphoreType.DMA((copies,)), pltpu.SemaphoreType.DMA((copies,)), pltpu.SemaphoreType.DMA],
        compiler_params=pltpu.CompilerParams(collective_id=ident, has_side_effects=True, vmem_limit_bytes=24 * MIB),
        cost_estimate=pl.CostEstimate(flops=rows * 2000, bytes_accessed=80_000_000, transcendentals=0),
    )(operand)


def sum_all(part, ident):
    rows = part.shape[0]
    size = rows // CHUNKS
    scratch = [pltpu.VMEM((CHUNKS, size // 2, BLOCK), F32), pltpu.VMEM((1, rows, BLOCK), F32)] + scatter_scratch(CHUNKS, size) + [pltpu.VMEM((CHUNKS, 6, size // 64, BLOCK), F32)]
    return comm_call(sum_kernel, rows, part, (1, rows, BLOCK), scratch, 22 * CHUNKS, ident)


def stack_planes(part, ident):
    rows = part.shape[0]
    scratch = [pltpu.VMEM((1, rows // 2, BLOCK), F32), pltpu.VMEM((4, rows // 8, BLOCK), F32)] + scatter_scratch(1, rows)
    return comm_call(stack_kernel, rows, part, (4, rows // 8, BLOCK), scratch, 8, ident)


def spread_planes(mine, ident):
    rows = mine.shape[1] * 8
    return comm_call(spread_kernel, rows, mine, (4, rows, BLOCK), [pltpu.VMEM((4, rows, BLOCK), F32)], 10, ident)


def lower_back(up, inv, x_ref, x0, base):
    for k in range(PAIR // PANEL - 1, -1, -1):
        a, b = k * PANEL, (k + 1) * PANEL
        v = base(a, b)
        if b < PAIR:
            v = v - jnp.sum(up[a:b, b:PAIR] * x_ref[0:1, x0 + b:x0 + PAIR], axis=1, keepdims=True)
        x_ref[0:1, x0 + a:x0 + b] = jnp.sum(inv[k] * v, axis=0, keepdims=True)


def load_half(planes, stage, sems, first, up, ridge):
    copies = [pltpu.make_async_copy(planes.at[first + i], stage.at[i], sems.at[i]) for i in range(2)]
    for copy in copies:
        copy.start()
    for copy in copies:
        copy.wait()
    diag = eye(BLOCK) * ridge
    for i in range(2):
        a, b = i * BLOCK, (i + 1) * BLOCK
        up[a:b, a:b] = stage[i, :BLOCK] + diag
        up[a:b, PAIR:] = stage[i, PAIR:].T


def low_kernel(planes, ridge, up, inv, stage, work, small, sems):
    load_half(planes, stage, sems, 0, up, ridge[0, 0])
    up[:BLOCK, BLOCK:PAIR] = stage[0, BLOCK:PAIR] + stage[1, BLOCK:PAIR]
    factor(up, inv, work, small, PAIR)


def high_kernel(planes, ridge, up_low, inv_low, cross, x_ref, stage, mid, up, inv, work, small, sems):
    load_half(planes, stage, sems, 2, up, ridge[0, 0])
    up[:BLOCK, BLOCK:PAIR] = cross[0, 2 * PAIR:2 * PAIR + BLOCK]
    for j in range(2):
        mid[:, j * BLOCK:(j + 1) * BLOCK] = cross[0, j * PAIR:(j + 1) * PAIR, :]
    mid[:, PAIR:] = up_low[:, PAIR:]
    panels = PAIR // PANEL
    for k in range(panels):
        a, b = k * PANEL, (k + 1) * PANEL
        mid[a:b, :PAIR] = dot(inv_low[k], mid[a:b, :PAIR])
        for i in range(k + 1, panels):
            c = i * PANEL
            mid[c:c + PANEL, :PAIR] = mid[c:c + PANEL, :PAIR] - dot(up_low[a:b, c:c + PANEL], mid[a:b, :PAIR], ((0,), (0,)))
    for i in range(panels):
        c = i * PANEL
        up[c:c + PANEL, c:] = up[c:c + PANEL, c:] - dot(mid[:, c:c + PANEL], mid[:, c:], ((0,), (0,)))
    factor(up, inv, work, small, PAIR)
    lower_back(up, inv, x_ref, PAIR, lambda a, b: up[a:b, PAIR:PAIR + 1])
    lower_back(up_low, inv_low, x_ref, 0, lambda a, b: up_low[a:b, PAIR:PAIR + 1] - jnp.sum(
        mid[a:b, :PAIR] * x_ref[0:1, PAIR:], axis=1, keepdims=True))


VM = pl.BlockSpec(memory_space=pltpu.VMEM)
SM = pl.BlockSpec(memory_space=pltpu.SMEM)
HB = pl.BlockSpec(memory_space=pl.ANY)
PANELS_SHAPE = (PAIR // PANEL, PANEL, PANEL)


def factor_low(planes, ridge):
    rows = planes.shape[1]
    return pl.pallas_call(
        low_kernel,
        out_shape=(jax.ShapeDtypeStruct((PAIR, PAIR + EXTRA), F32), jax.ShapeDtypeStruct(PANELS_SHAPE, F32)),
        in_specs=[HB, SM],
        out_specs=(VM, VM),
        scratch_shapes=[pltpu.VMEM((2, rows, BLOCK), F32), pltpu.VMEM((HALF, 2 * HALF), F32), pltpu.VMEM((2, HALF, HALF), F32), pltpu.SemaphoreType.DMA((2,))],
        compiler_params=pltpu.CompilerParams(vmem_limit_bytes=24 * MIB),
        cost_estimate=pl.CostEstimate(flops=40_000_000_000, bytes_accessed=10_000_000, transcendentals=0),
        name="factor_low",
    )(planes, ridge)


def factor_high(planes, ridge, up_low, inv_low, cross):
    rows = planes.shape[1]
    return pl.pallas_call(
        high_kernel,
        out_shape=jax.ShapeDtypeStruct((1, 2 * PAIR), F32),
        in_specs=[HB, SM, VM, VM, VM],
        out_specs=VM,
        scratch_shapes=[
            pltpu.VMEM((2, rows, BLOCK), F32),
            pltpu.VMEM((PAIR, PAIR + EXTRA), F32),
            pltpu.VMEM((PAIR, PAIR + EXTRA), F32),
            pltpu.VMEM(PANELS_SHAPE, F32),
            pltpu.VMEM((HALF, 2 * HALF), F32),
            pltpu.VMEM((2, HALF, HALF), F32),
            pltpu.SemaphoreType.DMA((2,)),
        ],
        compiler_params=pltpu.CompilerParams(vmem_limit_bytes=30 * MIB),
        cost_estimate=pl.CostEstimate(flops=50_000_000_000, bytes_accessed=10_000_000, transcendentals=0),
        name="factor_high",
    )(planes, ridge, up_low, inv_low, cross)


CROSS_ROWS = 2048


def cross_kernel(early, has_pair, has_prev, own, mate_lo, mate_hi, far_c, far_d, *refs):
    out, panel = refs[-2:]
    z = lax.axis_index('tp')
    mate, even, other = z_peers(z)

    def column(index):
        return pl.ds(pl.multiple_of(index * BLOCK, BLOCK), BLOCK)

    @pl.when(pl.program_id(0) == 0)
    def _():
        out[...] = refs[-3][...] if has_prev else jnp.zeros((CROSS_ROWS, BLOCK), F32)
        if has_pair:
            out[2 * PAIR:2 * PAIR + BLOCK] += refs[0][...]

    @pl.when(z == (1 if early else 0))
    def _():
        panel[:, column(z)] = own[...]
        panel[:, column(even)] = far_d[...]
        panel[:, column(other)] = far_c[...]
        panel[:, column(mate)] = mate_lo[...]
        for j in range(2):
            a = j * PAIR
            out[a:a + PAIR] += dot(panel[:, :PAIR], panel[:, PAIR + j * BLOCK:PAIR + (j + 1) * BLOCK], ((0,), (0,)))

    @pl.when(z >= 2)
    def _():
        panel[:, column(z)] = own[...]
        panel[:, column(even)] = far_d[...]
        panel[:, column(other)] = far_c[...]
        panel[:, column(mate)] = mate_hi[...]
        i = 1 if early else 0
        for j in range(2):
            a = j * PAIR + i * BLOCK
            out[a:a + BLOCK] += dot(panel[:, i * BLOCK:(i + 1) * BLOCK], panel[:, PAIR + j * BLOCK:PAIR + (j + 1) * BLOCK], ((0,), (0,)))
        if early:
            out[2 * PAIR:2 * PAIR + BLOCK] += dot(panel[:, PAIR:PAIR + BLOCK], panel[:, PAIR + BLOCK:], ((0,), (0,)))


def cross_gram(early, row0, own, mate_lo, mate_hi, far_c, far_d, prev=None, pair=None):
    rows = far_c.shape[0]
    tile = 256
    steps = rows // tile
    shift = row0 // tile
    near = pl.BlockSpec((tile, BLOCK), lambda i: (i + shift, 0))
    far = pl.BlockSpec((tile, BLOCK), lambda i: (i, 0))
    extras = [a for a in (pair, prev) if a is not None]

    return pl.pallas_call(
        functools.partial(cross_kernel, early, pair is not None, prev is not None),
        out_shape=jax.ShapeDtypeStruct((CROSS_ROWS, BLOCK), F32),
        grid=(steps,),
        in_specs=[near, near, near, far, far] + [pl.BlockSpec(a.shape, lambda i: (0, 0)) for a in extras],
        out_specs=pl.BlockSpec((CROSS_ROWS, BLOCK), lambda i: (0, 0)),
        scratch_shapes=[pltpu.VMEM((tile, 2 * PAIR), F32)],
        compiler_params=pltpu.CompilerParams(dimension_semantics=("arbitrary",), vmem_limit_bytes=24 * MIB),
        cost_estimate=pl.CostEstimate(flops=rows * 6_000_000, bytes_accessed=rows * 8000, transcendentals=0),
        name="cross_gram",
    )(own, mate_lo, mate_hi, far_c, far_d, *extras)


def pair_kernel(low, count, *refs):
    nears, mates, heads, out = refs[:count], refs[count:2 * count], refs[2 * count:-1], refs[-1]
    z = lax.axis_index('tp')
    r = BLOCK if low else 0

    @pl.when(pl.program_id(0) == 0)
    def _():
        if len(heads) == 1:
            out[...] = heads[0][...]
        elif low:
            out[:BLOCK] = heads[0][...]
            out[BLOCK:PAIR] = jnp.zeros((BLOCK, BLOCK), F32)
            out[PAIR:] = jnp.broadcast_to(heads[1][...], (EXTRA, BLOCK))
        else:
            out[...] = jnp.zeros((BLOCK, BLOCK), F32)

    mine = z < 2 if low else z >= 2
    for odd in range(2):
        @pl.when(mine & (lax.rem(z, 2) == odd))
        def _():
            for near, mate in zip(nears, mates):
                one, two = (mate, near) if odd else (near, mate)
                out[r:r + BLOCK] += dot(one[...], two[...], ((0,), (0,)))


def pair_gram(low, nears, mates, heads):
    rows = mates[0].shape[0]
    tile = 256
    out_rows = PAIR + EXTRA if low else BLOCK
    rolling = pl.BlockSpec((tile, BLOCK), lambda i: (i, 0))
    return pl.pallas_call(
        functools.partial(pair_kernel, low, len(nears)),
        out_shape=jax.ShapeDtypeStruct((out_rows, BLOCK), F32),
        grid=(rows // tile,),
        in_specs=[rolling] * (2 * len(nears)) + [pl.BlockSpec(h.shape, lambda i: (0, 0)) for h in heads],
        out_specs=pl.BlockSpec((out_rows, BLOCK), lambda i: (0, 0)),
        compiler_params=pltpu.CompilerParams(dimension_semantics=("arbitrary",), vmem_limit_bytes=24 * MIB),
        cost_estimate=pl.CostEstimate(flops=rows * 3_000_000 * len(nears), bytes_accessed=rows * 6000, transcendentals=0),
        name="pair_gram",
    )(*nears, *mates, *heads)


def residual_kernel(steps, design, x_ref, target, out, fits, send_sem, recv_sem):
    z, dp = lax.axis_index('tp'), lax.axis_index('dp')
    i = pl.program_id(0)
    tile = design.shape[0]
    peers = [{'tp': p, 'dp': dp} for p in z_peers(z)]

    @pl.when(i == 0)
    def _():
        barrier = pltpu.get_barrier_semaphore()
        for peer in peers:
            pl.semaphore_signal(barrier, inc=1, device_id=peer, device_id_type=MESH)
        pl.semaphore_wait(barrier, 3)

    x = [x_ref[0:1, pl.ds(pl.multiple_of(z * BLOCK + c * HALF, HALF), HALF)] for c in range(BLOCK // HALF)]
    rows = []
    for r in range(tile // HALF):
        t = sum(design[r * HALF:(r + 1) * HALF, c * HALF:(c + 1) * HALF] * x[c] for c in range(BLOCK // HALF))
        rows.append(jnp.sum(t.T, axis=0, keepdims=True))
    per = tile // HALF
    fits[0, pl.ds(pl.multiple_of(i * per, per), per), :] = jnp.concatenate(rows, axis=0)

    @pl.when(i == steps - 1)
    def _():
        copies = []
        for j, peer in enumerate(peers):
            copy = pltpu.make_async_remote_copy(src_ref=fits.at[0], dst_ref=fits.at[j + 1], send_sem=send_sem.at[j], recv_sem=recv_sem.at[j], device_id=peer, device_id_type=MESH)
            copy.start()
            copies.append(copy)
        for copy in copies:
            copy.wait()
        lo = jnp.where(z % 2 == 0, fits[0] + fits[1], fits[1] + fits[0])
        hi = jnp.where(z % 2 == 0, fits[2] + fits[3], fits[3] + fits[2])
        out[...] = target[...] - (lo + hi)


def residual(design_blk, x_row, target_tile):
    rows = design_blk.shape[0]
    tile = 1024
    steps = rows // tile
    whole = pl.BlockSpec(target_tile.shape, lambda i: (0, 0))
    return pl.pallas_call(
        functools.partial(residual_kernel, steps),
        out_shape=jax.ShapeDtypeStruct(target_tile.shape, F32),
        grid=(steps,),
        in_specs=[pl.BlockSpec((tile, BLOCK), lambda i: (i, 0)), pl.BlockSpec(x_row.shape, lambda i: (0, 0)), whole],
        out_specs=whole,
        scratch_shapes=[pltpu.VMEM((4,) + target_tile.shape, F32), pltpu.SemaphoreType.DMA((3,)), pltpu.SemaphoreType.DMA((3,))],
        compiler_params=pltpu.CompilerParams(collective_id=3, has_side_effects=True, dimension_semantics=("arbitrary",), vmem_limit_bytes=24 * MIB),
        cost_estimate=pl.CostEstimate(flops=6_000_000_000, bytes_accessed=13_000_000, transcendentals=0),
        name="residual",
    )(design_blk, x_row, target_tile)


EDGES = (0, 512, 1280, 2048)


def solution(mesh):
    col_ways, row_ways = mesh.shape['tp'], mesh.shape['dp']

    def swap(block, one, two):
        pairs = [(s * row_ways + d, t * row_ways + d) for s, t in ((one, two), (two, one)) for d in range(row_ways)]
        return lax.ppermute(block, ('tp', 'dp'), pairs)

    def local_fit(design_blk, target_blk, ridge):
        rows_dev, _ = design_blk.shape
        quarter_rows = rows_dev // col_ways
        z = lax.axis_index('tp')

        def piece(array, index):
            return lax.dynamic_slice_in_dim(array, index * quarter_rows, quarter_rows)

        to_mate = piece(design_blk, z ^ 1)
        to_mate, design_b = lax.optimization_barrier((to_mate, design_blk))
        low_a = swap(to_mate, 0, 1)
        to_third, to_even, own = piece(design_b, z ^ 3), piece(design_b, z ^ 2), piece(design_b, z)
        low_b = swap(to_third, 0, 1)
        near_c = swap(to_third, 1, 2)
        near_d = swap(to_even, 1, 3)
        high_a = swap(to_mate, 2, 3)
        to_third_b, to_even_b, own = lax.optimization_barrier((to_third, to_even, own))
        chunks = [(to_third_b[i:j], to_even_b[i:j]) for i, j in zip(EDGES, EDGES[1:])]
        own_gram = dot(design_b, design_b, ((0,), (0,)))
        moment = dot(target_blk[None, :], design_b)
        part = pair_gram(True, (own,), (low_a,), (own_gram, moment))
        low_a, low_b, near_c, near_d, part, chunks = lax.optimization_barrier(
            (low_a, low_b, near_c, near_d, part, chunks))
        far_c, far_d = [], []

        def send_late(pieces):
            far_c.append(swap(pieces[0], 0, 3))
            far_d.append(swap(pieces[1], 0, 2))

        send_late(chunks[0])
        part = pair_gram(True, (to_even,), (low_b,), (part,))
        mine = stack_planes(part, 1)
        mine, late_b, chunks = lax.optimization_barrier((mine, to_third, chunks))
        send_late(chunks[1])
        high_b = swap(late_b, 2, 3)
        send_late(chunks[2])
        planes = spread_planes(mine, 2)
        ridge_cell = jnp.reshape(ridge, (1, 1))
        up_low, inv_low = factor_low(planes, ridge_cell)
        own_b, near_c, up_low = lax.optimization_barrier((own, near_c, up_low))
        cross = cross_gram(True, 0, own_b, low_a, high_a, near_c, near_d)
        cross = cross_gram(False, EDGES[0], own_b, low_a, high_a, far_c[0], far_d[0], cross)
        cross = cross_gram(False, EDGES[1], own_b, low_a, high_a, far_c[1], far_d[1], cross)
        high_b, cross = lax.optimization_barrier((high_b, cross))
        pair_high = pair_gram(False, (to_even,), (high_b,), ())
        cross = cross_gram(False, EDGES[2], own_b, low_a, high_a, far_c[2], far_d[2], cross, pair_high)
        cross = sum_all(cross, 4)
        x_row = factor_high(planes, ridge_cell, up_low, inv_low, cross)
        left = residual(design_b, x_row, jnp.reshape(target_blk, (rows_dev // HALF, HALF)))
        return x_row[0], jnp.reshape(left, (rows_dev,))

    return jax.shard_map(local_fit, mesh=mesh, in_specs=(P('dp', 'tp'), P('dp'), P()), out_specs=(P(), P('dp')), check_vma=False)
```

```python
import functools
import jax
import jax.numpy as jnp
from jax import lax
from jax.experimental import pallas as pl
from jax.experimental.pallas import tpu as pltpu
from jax.sharding import PartitionSpec as P

HIGHEST = lax.Precision.HIGHEST
F32 = jnp.float32
SUB, HALF, PANEL, BLOCK, EXTRA = 16, 128, 256, 384, 128
PAIR = 2 * BLOCK
MESH = pl.DeviceIdType.MESH
MIB = 1024 * 1024


def dot(a, b, dims=((1,), (0,))):
    return lax.dot_general(a, b, (dims, ((), ())), precision=HIGHEST, preferred_element_type=F32)


def row_blocks(work, r):
    return work[r:r + SUB, :HALF], work[r:r + SUB, HALF:]


def lanes(block, col0):
    return [jnp.broadcast_to(block[:, col0 + c:col0 + c + 1], (SUB, HALF)) for c in range(SUB)]


def invert_factor(work, inv_ref):
    rows = lax.broadcasted_iota(jnp.int32, (SUB, HALF), 0)
    left, right = row_blocks(work, 0)
    for r in range(0, HALF, SUB):
        more = r + SUB < HALF
        cols = lanes(left, r)
        if more:
            next_left, next_right = row_blocks(work, r + SUB)
            below = lanes(next_left, r)
        pivots = cols[0]
        for p in range(SUB):
            inv = 1.0 / cols[p][p:p + 1, :]
            fac = jnp.where(rows > p, cols[p] * inv, 0.0)
            left_row, right_row = left[p:p + 1, :], right[p:p + 1, :]
            left, right = left - fac * left_row, right - fac * right_row
            if more:
                low = below[p] * inv
                next_left, next_right = next_left - low * left_row, next_right - low * right_row
            for c in range(p + 1, SUB):
                entry = cols[c][p:p + 1, :]
                cols[c] = cols[c] - fac * entry
                if more:
                    below[c] = below[c] - low * entry
            pivots = jnp.where(rows == p, cols[p], pivots)
        scale = lax.rsqrt(pivots)
        left, right = left * scale, right * scale
        inv_ref[r:r + SUB, :] = right
        if r + 2 * SUB < HALF:
            upd = dot(left, jnp.concatenate([left, right], axis=1), ((0,), (0,)))
            work[r + 2 * SUB:, :] = work[r + 2 * SUB:, :] - upd[r + 2 * SUB:, :]
        if more:
            left, right = next_left, next_right


def eye(n):
    rows = lax.broadcasted_iota(jnp.int32, (n, n), 0)
    return jnp.where(rows == lax.broadcasted_iota(jnp.int32, (n, n), 1), 1.0, 0.0).astype(F32)


def factor(up, inv, work, small, n):
    panels = n // PANEL
    first, carry = small.at[0], small.at[1]

    def step(t, _):
        k, odd = t // 2, lax.rem(t, 2)
        r0 = pl.multiple_of(t * HALF, HALF)
        r1 = pl.multiple_of(t * HALF + HALF * (1 - odd), HALF)
        work[:, :HALF] = up[pl.ds(r0, HALF), pl.ds(r0, HALF)]
        work[:, HALF:] = eye(HALF)
        invert_factor(work, first)

        @pl.when(odd == 0)
        def _():
            w1 = first[...]
            inv[k] = jnp.zeros((PANEL, PANEL), F32)
            inv[k, :HALF, :HALF] = w1
            u12 = dot(w1, up[pl.ds(r0, HALF), pl.ds(r1, HALF)])
            both = dot(u12, jnp.concatenate([u12, w1], axis=1), ((0,), (0,)))
            up[pl.ds(r1, HALF), pl.ds(r1, HALF)] = up[pl.ds(r1, HALF), pl.ds(r1, HALF)] - both[:, :HALF]
            carry[...] = both[:, HALF:]

        @pl.when(odd == 1)
        def _():
            w2 = first[...]
            inv[k, HALF:, HALF:] = w2
            inv[k, HALF:, :HALF] = -dot(w2, carry[...])

        for kk in range(panels):
            @pl.when(t == 2 * kk + 1)
            def _():
                a, b = kk * PANEL, (kk + 1) * PANEL
                up[a:b, b:] = dot(inv[kk], up[a:b, b:])
                for i in range(kk + 1, panels):
                    c = i * PANEL
                    up[c:c + PANEL, c:] = up[c:c + PANEL, c:] - dot(up[a:b, c:c + PANEL], up[a:b, c:], ((0,), (0,)))
        return 0

    lax.fori_loop(0, 2 * panels, step, 0)


def places():
    z, dp = lax.axis_index('tp'), lax.axis_index('dp')
    core, x, y = lax.rem(dp, 2), lax.rem(dp // 2, 2), dp // 4
    return z, dp, core, x, y


def z_peers(z):
    return (z + 1 - 2 * lax.rem(z, 2), z + 2 - 4 * (z // 2), 3 - z)


def plane_peers(z, dp, core, x, y):
    return ({'tp': z, 'dp': dp + 1 - 2 * core}, {'tp': z, 'dp': dp + 2 - 4 * x}, {'tp': z, 'dp': dp + 4 - 8 * y})


def meet(peers):
    barrier = pltpu.get_barrier_semaphore()
    for peer in peers:
        pl.semaphore_signal(barrier, inc=1, device_id=peer, device_id_type=MESH)
    pl.semaphore_wait(barrier, len(peers))


def starter(send_sem, recv_sem):
    count = [0]

    def start(src, dst, peer):
        i = count[0]
        count[0] += 1
        copy = pltpu.make_async_remote_copy(src_ref=src, dst_ref=dst, send_sem=send_sem.at[i], recv_sem=recv_sem.at[i], device_id=peer, device_id_type=MESH)
        copy.start()
        return copy

    return start


def at(base, size):
    return pl.ds(pl.multiple_of(base, 8), size)


def spans(rows, core, x, y):
    half, quart, eighth, sixt = rows // 2, rows // 4, rows // 8, rows // 16
    a1, b1 = x * eighth, quart + y * eighth
    return core * half, a1, b1, a1 + y * sixt, b1 + x * sixt


def plane_scatter(rows, part, acc, got, start, peers, where):
    _, _, core, x, y = where
    core_peer, x_peer, y_peer = peers
    half, quart, eighth, sixt = rows // 2, rows // 4, rows // 8, rows // 16
    own, a1, b1, a2, b2 = spans(rows, core, x, y)
    got_core, got_a, got_b, got_a2, got_b2 = got
    copy = start(part.at[at((1 - core) * half, half)], got_core, core_peer)
    yield
    copy.wait()
    acc[...] = part[at(own, half)] + got_core[...]
    copies = [start(acc.at[at((1 - x) * eighth, eighth)], got_a, x_peer), start(acc.at[at(quart + (1 - y) * eighth, eighth)], got_b, y_peer)]
    yield
    copies[0].wait()
    acc[at(a1, eighth)] = acc[at(a1, eighth)] + got_a[...]
    copies[1].wait()
    acc[at(b1, eighth)] = acc[at(b1, eighth)] + got_b[...]
    copies = [start(acc.at[at(a1 + (1 - y) * sixt, sixt)], got_a2, y_peer), start(acc.at[at(b1 + (1 - x) * sixt, sixt)], got_b2, x_peer)]
    yield
    copies[0].wait()
    acc[at(a2, sixt)] = acc[at(a2, sixt)] + got_a2[...]
    copies[1].wait()
    acc[at(b2, sixt)] = acc[at(b2, sixt)] + got_b2[...]


def plane_gather(rows, full, start, peers, where):
    _, _, core, x, y = where
    core_peer, x_peer, y_peer = peers
    half, eighth, sixt = rows // 2, rows // 8, rows // 16
    own, a1, b1, a2, b2 = spans(rows, core, x, y)
    for sizes in (((a2, sixt, y_peer), (b2, sixt, x_peer)), ((a1, eighth, x_peer), (b1, eighth, y_peer)), ((0, half, core_peer),)):
        copies = []
        for base, size, peer in sizes:
            ref = full.at[:, at(own + base, size)]
            copies.append(start(ref, ref, peer))
        yield
        for copy in copies:
            copy.wait()


def in_turn(chunks):
    chunks = list(chunks)
    while chunks:
        chunks = [chunk for chunk in chunks if next(chunk, chunks) is not chunks]


def wait_all(copies):
    for copy in copies:
        copy.wait()


def sum_chunk(rows, part, acc, full, got, got_z, start, peers, z_peer, where):
    z, _, core, x, y = where
    yield from plane_scatter(rows, part, acc, got, start, peers, where)
    own, _, _, a2, b2 = spans(rows, core, x, y)
    share = rows // 64
    copies = []
    for k, piece in enumerate((a2, b2)):
        for j, peer in enumerate(z_peer):
            copies.append(start(acc.at[at(piece + peer['tp'] * share, share)], got_z.at[2 * j + k], peer))
    yield
    wait_all(copies)
    copies = []
    for k, piece in enumerate((a2, b2)):
        mine = piece + z * share
        full[0, at(own + mine, share)] = (acc[at(mine, share)] + got_z[k]) + (got_z[2 + k] + got_z[4 + k])
        ref = full.at[0, at(own + mine, share)]
        copies += [start(ref, ref, peer) for peer in z_peer]
    yield
    wait_all(copies)
    yield from plane_gather(rows, full, start, peers, where)


CHUNKS = 4


def sum_kernel(rows, part, out, acc, full, g0, g1, g2, g3, g4, got_z, send_sem, recv_sem, out_sem):
    where = places()
    z, dp = where[:2]
    peers = plane_peers(*where)
    z_peer = [{'tp': p, 'dp': dp} for p in z_peers(z)]
    meet(list(peers) + z_peer)
    start = starter(send_sem, recv_sem)
    size = rows // CHUNKS
    in_turn(sum_chunk(size, part.at[c * size:(c + 1) * size], acc.at[c], full.at[:, c * size:(c + 1) * size],
                      [g.at[c] for g in (g0, g1, g2, g3, g4)], got_z.at[c], start, peers, z_peer, where) for c in range(CHUNKS))
    copy = pltpu.make_async_copy(full, out, out_sem)
    copy.start()
    copy.wait()


def stack_kernel(rows, part, out, acc, mine, g0, g1, g2, g3, g4, send_sem, recv_sem, out_sem):
    where = places()
    z, dp, core, x, y = where
    peers = plane_peers(*where)
    z_peer = [{'tp': p, 'dp': dp} for p in z_peers(z)]
    meet(list(peers) + z_peer)
    start = starter(send_sem, recv_sem)
    in_turn([plane_scatter(rows, part, acc.at[0], [g.at[0] for g in (g0, g1, g2, g3, g4)], start, peers, where)])
    _, _, _, a2, b2 = spans(rows, core, x, y)
    sixt = rows // 16
    mine[z, :sixt] = acc[0, at(a2, sixt)]
    mine[z, sixt:] = acc[0, at(b2, sixt)]
    wait_all([start(mine.at[z], mine.at[z], peer) for peer in z_peer])
    copy = pltpu.make_async_copy(mine, out, out_sem)
    copy.start()
    copy.wait()


def spread_kernel(rows, mine, out, full, send_sem, recv_sem, out_sem):
    where = places()
    _, _, core, x, y = where
    peers = plane_peers(*where)
    meet(peers)
    own, _, _, a2, b2 = spans(rows, core, x, y)
    sixt = rows // 16
    full[:, at(own + a2, sixt)] = mine[:, :sixt]
    full[:, at(own + b2, sixt)] = mine[:, sixt:]
    start = starter(send_sem, recv_sem)
    in_turn(plane_gather(rows, full.at[2 * c:2 * c + 2], start, peers, where) for c in range(2))
    copy = pltpu.make_async_copy(full, out, out_sem)
    copy.start()
    copy.wait()


def scatter_scratch(chunks, rows):
    return [pltpu.VMEM((chunks, rows // d, BLOCK), F32) for d in (2, 8, 8, 16, 16)]


def comm_call(body, rows, operand, out_shape, scratch, copies, ident):
    return pl.pallas_call(
        functools.partial(body, rows),
        out_shape=jax.ShapeDtypeStruct(out_shape, F32),
        in_specs=[pl.BlockSpec(memory_space=pltpu.VMEM)],
        out_specs=pl.BlockSpec(memory_space=pl.ANY),
        scratch_shapes=scratch + [pltpu.SemaphoreType.DMA((copies,)), pltpu.SemaphoreType.DMA((copies,)), pltpu.SemaphoreType.DMA],
        compiler_params=pltpu.CompilerParams(collective_id=ident, has_side_effects=True, vmem_limit_bytes=24 * MIB),
        cost_estimate=pl.CostEstimate(flops=rows * 2000, bytes_accessed=80_000_000, transcendentals=0),
    )(operand)


def sum_all(part, ident):
    rows = part.shape[0]
    size = rows // CHUNKS
    scratch = [pltpu.VMEM((CHUNKS, size // 2, BLOCK), F32), pltpu.VMEM((1, rows, BLOCK), F32)] + scatter_scratch(CHUNKS, size) + [pltpu.VMEM((CHUNKS, 6, size // 64, BLOCK), F32)]
    return comm_call(sum_kernel, rows, part, (1, rows, BLOCK), scratch, 22 * CHUNKS, ident)


def stack_planes(part, ident):
    rows = part.shape[0]
    scratch = [pltpu.VMEM((1, rows // 2, BLOCK), F32), pltpu.VMEM((4, rows // 8, BLOCK), F32)] + scatter_scratch(1, rows)
    return comm_call(stack_kernel, rows, part, (4, rows // 8, BLOCK), scratch, 8, ident)


def spread_planes(mine, ident):
    rows = mine.shape[1] * 8
    return comm_call(spread_kernel, rows, mine, (4, rows, BLOCK), [pltpu.VMEM((4, rows, BLOCK), F32)], 10, ident)


def lower_back(up, inv, x_ref, x0, base):
    for k in range(PAIR // PANEL - 1, -1, -1):
        a, b = k * PANEL, (k + 1) * PANEL
        v = base(a, b)
        if b < PAIR:
            v = v - jnp.sum(up[a:b, b:PAIR] * x_ref[0:1, x0 + b:x0 + PAIR], axis=1, keepdims=True)
        x_ref[0:1, x0 + a:x0 + b] = jnp.sum(inv[k] * v, axis=0, keepdims=True)


def fetch_half(planes, stage, sems, first):
    copies = [pltpu.make_async_copy(planes.at[first + i], stage.at[i], sems.at[i]) for i in range(2)]
    for copy in copies:
        copy.start()
    return copies


def fill_half(copies, stage, up, ridge):
    wait_all(copies)
    diag = eye(BLOCK) * ridge
    for i in range(2):
        a, b = i * BLOCK, (i + 1) * BLOCK
        up[a:b, a:b] = stage[i, :BLOCK] + diag
        up[a:b, PAIR:] = stage[i, PAIR:].T


def low_kernel(planes, ridge, up, inv, stage, work, small, sems):
    fill_half(fetch_half(planes, stage, sems, 0), stage, up, ridge[0, 0])
    up[:BLOCK, BLOCK:PAIR] = stage[0, BLOCK:PAIR] + stage[1, BLOCK:PAIR]
    factor(up, inv, work, small, PAIR)


def high_kernel(planes, ridge, up_low, inv_low, cross, design, x_ref, fits, stage, mid, up, inv, work, small, rows, sems):
    copies = fetch_half(planes, stage, sems, 2)
    fetch = pltpu.make_async_copy(design, rows, sems.at[2])
    fetch.start()
    for j in range(2):
        mid[:, j * BLOCK:(j + 1) * BLOCK] = cross[0, j * PAIR:(j + 1) * PAIR, :]
    mid[:, PAIR:] = up_low[:, PAIR:]
    panels = PAIR // PANEL
    for k in range(panels):
        a, b = k * PANEL, (k + 1) * PANEL
        mid[a:b, :PAIR] = dot(inv_low[k], mid[a:b, :PAIR])
        for i in range(k + 1, panels):
            c = i * PANEL
            mid[c:c + PANEL, :PAIR] = mid[c:c + PANEL, :PAIR] - dot(up_low[a:b, c:c + PANEL], mid[a:b, :PAIR], ((0,), (0,)))
    fill_half(copies, stage, up, ridge[0, 0])
    up[:BLOCK, BLOCK:PAIR] = cross[0, 2 * PAIR:2 * PAIR + BLOCK]
    for i in range(panels):
        c = i * PANEL
        up[c:c + PANEL, c:] = up[c:c + PANEL, c:] - dot(mid[:, c:c + PANEL], mid[:, c:], ((0,), (0,)))
    factor(up, inv, work, small, PAIR)
    lower_back(up, inv, x_ref, PAIR, lambda a, b: up[a:b, PAIR:PAIR + 1])
    lower_back(up_low, inv_low, x_ref, 0, lambda a, b: up_low[a:b, PAIR:PAIR + 1] - jnp.sum(
        mid[a:b, :PAIR] * x_ref[0:1, PAIR:], axis=1, keepdims=True))
    fetch.wait()
    z = lax.axis_index('tp')
    x = [x_ref[0:1, pl.ds(pl.multiple_of(z * BLOCK + c * HALF, HALF), HALF)] for c in range(BLOCK // HALF)]
    group = 8

    def fit_rows(g, _):
        lines = []
        for r in range(group):
            base = pl.multiple_of((g * group + r) * HALF, HALF)
            t = sum(rows[pl.ds(base, HALF), c * HALF:(c + 1) * HALF] * x[c] for c in range(BLOCK // HALF))
            lines.append(jnp.sum(t.T, axis=0, keepdims=True))
        fits[pl.ds(pl.multiple_of(g * group, group), group), :] = jnp.concatenate(lines, axis=0)
        return 0

    lax.fori_loop(0, fits.shape[0] // group, fit_rows, 0)


VM = pl.BlockSpec(memory_space=pltpu.VMEM)
SM = pl.BlockSpec(memory_space=pltpu.SMEM)
HB = pl.BlockSpec(memory_space=pl.ANY)
PANELS_SHAPE = (PAIR // PANEL, PANEL, PANEL)


def factor_low(planes, ridge):
    rows = planes.shape[1]
    return pl.pallas_call(
        low_kernel,
        out_shape=(jax.ShapeDtypeStruct((PAIR, PAIR + EXTRA), F32), jax.ShapeDtypeStruct(PANELS_SHAPE, F32)),
        in_specs=[HB, SM],
        out_specs=(VM, VM),
        scratch_shapes=[pltpu.VMEM((2, rows, BLOCK), F32), pltpu.VMEM((HALF, 2 * HALF), F32), pltpu.VMEM((2, HALF, HALF), F32), pltpu.SemaphoreType.DMA((2,))],
        compiler_params=pltpu.CompilerParams(vmem_limit_bytes=24 * MIB),
        cost_estimate=pl.CostEstimate(flops=40_000_000_000, bytes_accessed=10_000_000, transcendentals=0),
        name="factor_low",
    )(planes, ridge)


def factor_high(planes, ridge, up_low, inv_low, cross, design_blk):
    rows = planes.shape[1]
    lines = design_blk.shape[0] // HALF
    return pl.pallas_call(
        high_kernel,
        out_shape=(jax.ShapeDtypeStruct((1, 2 * PAIR), F32), jax.ShapeDtypeStruct((lines, HALF), F32)),
        in_specs=[HB, SM, VM, VM, VM, HB],
        out_specs=(VM, VM),
        scratch_shapes=[
            pltpu.VMEM((2, rows, BLOCK), F32),
            pltpu.VMEM((PAIR, PAIR + EXTRA), F32),
            pltpu.VMEM((PAIR, PAIR + EXTRA), F32),
            pltpu.VMEM(PANELS_SHAPE, F32),
            pltpu.VMEM((HALF, 2 * HALF), F32),
            pltpu.VMEM((2, HALF, HALF), F32),
            pltpu.VMEM(design_blk.shape, F32),
            pltpu.SemaphoreType.DMA((3,)),
        ],
        compiler_params=pltpu.CompilerParams(vmem_limit_bytes=42 * MIB),
        cost_estimate=pl.CostEstimate(flops=50_000_000_000, bytes_accessed=10_000_000, transcendentals=0),
        name="factor_high",
    )(planes, ridge, up_low, inv_low, cross, design_blk)


CROSS_ROWS = 2048


def cross_kernel(early, has_pair, has_prev, own, mate_lo, mate_hi, far_c, far_d, *refs):
    out, panel = refs[-2:]
    z = lax.axis_index('tp')
    mate, even, other = z_peers(z)

    def column(index):
        return pl.ds(pl.multiple_of(index * BLOCK, BLOCK), BLOCK)

    @pl.when(pl.program_id(0) == 0)
    def _():
        out[...] = refs[-3][...] if has_prev else jnp.zeros((CROSS_ROWS, BLOCK), F32)
        if has_pair:
            out[2 * PAIR:2 * PAIR + BLOCK] += refs[0][...]

    full = 1 if early else 0
    panel[:, column(z)] = own[...]
    panel[:, column(even)] = far_d[...]
    panel[:, column(other)] = far_c[...]

    @pl.when(z < 2)
    def _():
        panel[:, column(mate)] = mate_lo[...]

    @pl.when(z >= 2)
    def _():
        panel[:, column(mate)] = mate_hi[...]

    @pl.when((z == full) | (z >= 2))
    def _():
        def row_block(i, _):
            low = panel[:, column(i)]
            for j in range(2):
                a = pl.multiple_of(j * PAIR + i * BLOCK, BLOCK)
                hi = panel[:, PAIR + j * BLOCK:PAIR + (j + 1) * BLOCK]
                out[pl.ds(a, BLOCK)] += dot(low, hi, ((0,), (0,)))
            return 0

        lax.fori_loop(jnp.where(z < 2, 0, full), jnp.where(z < 2, 2, full + 1), row_block, 0)

    if early:
        @pl.when(z >= 2)
        def _():
            out[2 * PAIR:2 * PAIR + BLOCK] += dot(panel[:, PAIR:PAIR + BLOCK], panel[:, PAIR + BLOCK:], ((0,), (0,)))


def cross_gram(early, row0, own, mate_lo, mate_hi, far_c, far_d, prev=None, pair=None):
    rows = far_c.shape[0]
    tile = 256
    steps = rows // tile
    shift = row0 // tile
    near = pl.BlockSpec((tile, BLOCK), lambda i: (i + shift, 0))
    far = pl.BlockSpec((tile, BLOCK), lambda i: (i, 0))
    extras = [a for a in (pair, prev) if a is not None]

    return pl.pallas_call(
        functools.partial(cross_kernel, early, pair is not None, prev is not None),
        out_shape=jax.ShapeDtypeStruct((CROSS_ROWS, BLOCK), F32),
        grid=(steps,),
        in_specs=[near, near, near, far, far] + [pl.BlockSpec(a.shape, lambda i: (0, 0)) for a in extras],
        out_specs=pl.BlockSpec((CROSS_ROWS, BLOCK), lambda i: (0, 0)),
        scratch_shapes=[pltpu.VMEM((tile, 2 * PAIR), F32)],
        compiler_params=pltpu.CompilerParams(dimension_semantics=("arbitrary",), vmem_limit_bytes=24 * MIB),
        cost_estimate=pl.CostEstimate(flops=rows * 6_000_000, bytes_accessed=rows * 8000, transcendentals=0),
        name="cross_gram",
    )(own, mate_lo, mate_hi, far_c, far_d, *extras)


def pair_kernel(low, count, *refs):
    nears, mates, heads, out = refs[:count], refs[count:2 * count], refs[2 * count:-1], refs[-1]
    z = lax.axis_index('tp')
    r = BLOCK if low else 0

    @pl.when(pl.program_id(0) == 0)
    def _():
        if len(heads) == 1:
            out[...] = heads[0][...]
        elif low:
            out[:BLOCK] = heads[0][...]
            out[BLOCK:PAIR] = jnp.zeros((BLOCK, BLOCK), F32)
            out[PAIR:] = jnp.broadcast_to(heads[1][...], (EXTRA, BLOCK))
        else:
            out[...] = jnp.zeros((BLOCK, BLOCK), F32)

    mine = z < 2 if low else z >= 2
    for odd in range(2):
        @pl.when(mine & (lax.rem(z, 2) == odd))
        def _():
            for near, mate in zip(nears, mates):
                one, two = (mate, near) if odd else (near, mate)
                out[r:r + BLOCK] += dot(one[...], two[...], ((0,), (0,)))


def pair_gram(low, nears, mates, heads, row0=0):
    rows = mates[0].shape[0]
    tile = 256
    out_rows = PAIR + EXTRA if low else BLOCK
    shift = row0 // tile
    near = pl.BlockSpec((tile, BLOCK), lambda i: (i + shift, 0))
    far = pl.BlockSpec((tile, BLOCK), lambda i: (i, 0))
    return pl.pallas_call(
        functools.partial(pair_kernel, low, len(nears)),
        out_shape=jax.ShapeDtypeStruct((out_rows, BLOCK), F32),
        grid=(rows // tile,),
        in_specs=[near] * len(nears) + [far] * len(nears) + [pl.BlockSpec(h.shape, lambda i: (0, 0)) for h in heads],
        out_specs=pl.BlockSpec((out_rows, BLOCK), lambda i: (0, 0)),
        compiler_params=pltpu.CompilerParams(dimension_semantics=("arbitrary",), vmem_limit_bytes=24 * MIB),
        cost_estimate=pl.CostEstimate(flops=rows * 3_000_000 * len(nears), bytes_accessed=rows * 6000, transcendentals=0),
        name="pair_gram",
    )(*nears, *mates, *heads)


def residual_kernel(fit, target, out, got, send_sem, recv_sem):
    z, dp = lax.axis_index('tp'), lax.axis_index('dp')
    peers = [{'tp': p, 'dp': dp} for p in z_peers(z)]
    meet(peers)
    start = starter(send_sem, recv_sem)
    wait_all([start(fit, got.at[j], peer) for j, peer in enumerate(peers)])
    out[...] = target[...] - ((fit[...] + got[0]) + (got[1] + got[2]))


def residual(fits, target_tile):
    return pl.pallas_call(
        residual_kernel,
        out_shape=jax.ShapeDtypeStruct(target_tile.shape, F32),
        in_specs=[VM, VM],
        out_specs=VM,
        scratch_shapes=[pltpu.VMEM((3,) + target_tile.shape, F32), pltpu.SemaphoreType.DMA((3,)), pltpu.SemaphoreType.DMA((3,))],
        compiler_params=pltpu.CompilerParams(collective_id=3, has_side_effects=True),
        cost_estimate=pl.CostEstimate(flops=3_000_000_000, bytes_accessed=1_000_000, transcendentals=0),
        name="residual",
    )(fits, target_tile)


EDGES = (0, 512, 1536, 2048)


def solution(mesh):
    col_ways, row_ways = mesh.shape['tp'], mesh.shape['dp']

    def swap(block, one, two):
        pairs = [(s * row_ways + d, t * row_ways + d) for s, t in ((one, two), (two, one)) for d in range(row_ways)]
        return lax.ppermute(block, ('tp', 'dp'), pairs)

    def local_fit(design_blk, target_blk, ridge):
        rows_dev, _ = design_blk.shape
        quarter_rows = rows_dev // col_ways
        z = lax.axis_index('tp')

        def piece(array, index):
            return lax.dynamic_slice_in_dim(array, index * quarter_rows, quarter_rows)

        to_mate = piece(design_blk, z ^ 1)
        to_mate, design_b = lax.optimization_barrier((to_mate, design_blk))
        low_a = swap(to_mate, 0, 1)
        to_third = piece(design_b, z ^ 3)
        to_third, design_b = lax.optimization_barrier((to_third, design_b))
        to_even = piece(design_b, z ^ 2)
        low_b = swap(to_third, 0, 1)
        near_c = swap(to_third, 1, 2)
        near_d = swap(to_even, 1, 3)
        high_a = swap(to_mate, 2, 3)
        to_third_b, to_even_b, design_b = lax.optimization_barrier((to_third, to_even, design_b))
        own = piece(design_b, z)
        chunks = [(to_third_b[i:j], to_even_b[i:j]) for i, j in zip(EDGES, EDGES[1:])]
        late_b = to_third_b[EDGES[1]:]
        own_gram = dot(design_b, design_b, ((0,), (0,)))
        moment = dot(target_blk[None, :], design_b)
        part = pair_gram(True, (own,), (low_a,), (own_gram, moment))
        low_a, low_b, near_c, near_d, part, chunks = lax.optimization_barrier(
            (low_a, low_b, near_c, near_d, part, chunks))
        far_c, far_d = [], []

        def send_late(pieces):
            far_c.append(swap(pieces[0], 0, 3))
            far_d.append(swap(pieces[1], 0, 2))

        send_late(chunks[0])
        high_b0 = swap(chunks[0][0], 2, 3)
        part = pair_gram(True, (to_even,), (low_b,), (part,))
        mine = stack_planes(part, 1)
        mine, late_b, chunks = lax.optimization_barrier((mine, late_b, chunks))
        send_late(chunks[1])
        high_b1 = swap(late_b, 2, 3)
        send_late(chunks[2])
        planes = spread_planes(mine, 2)
        ridge_cell = jnp.reshape(ridge, (1, 1))
        up_low, inv_low = factor_low(planes, ridge_cell)
        own_b, near_c, up_low = lax.optimization_barrier((own, near_c, up_low))
        cross = cross_gram(True, 0, own_b, low_a, high_a, near_c, near_d)
        cross = cross_gram(False, EDGES[0], own_b, low_a, high_a, far_c[0], far_d[0], cross)
        pair_high = pair_gram(False, (to_even,), (high_b0,), ())
        cross = cross_gram(False, EDGES[1], own_b, low_a, high_a, far_c[1], far_d[1], cross)
        high_b1, cross = lax.optimization_barrier((high_b1, cross))
        pair_high = pair_gram(False, (to_even,), (high_b1,), (pair_high,), EDGES[1])
        cross = cross_gram(False, EDGES[2], own_b, low_a, high_a, far_c[2], far_d[2], cross, pair_high)
        cross = sum_all(cross, 4)
        x_row, fits = factor_high(planes, ridge_cell, up_low, inv_low, cross, design_b)
        left = residual(fits, jnp.reshape(target_blk, (rows_dev // HALF, HALF)))
        return x_row[0], jnp.reshape(left, (rows_dev,))

    return jax.shard_map(local_fit, mesh=mesh, in_specs=(P('dp', 'tp'), P('dp'), P()), out_specs=(P(), P('dp')), check_vma=False)
```

```python
import functools
import jax
import jax.numpy as jnp
from jax import lax
from jax.experimental import pallas as pl
from jax.experimental.pallas import tpu as pltpu
from jax.sharding import PartitionSpec as P

HIGHEST = lax.Precision.HIGHEST
F32 = jnp.float32
SUB, HALF, PANEL, BLOCK, EXTRA = 16, 128, 256, 384, 128
PAIR = 2 * BLOCK
MESH = pl.DeviceIdType.MESH
MIB = 1024 * 1024


def dot(a, b, dims=((1,), (0,))):
    return lax.dot_general(a, b, (dims, ((), ())), precision=HIGHEST, preferred_element_type=F32)


def row_blocks(work, r):
    return work[r:r + SUB, :HALF], work[r:r + SUB, HALF:]


def lanes(block, col0):
    return [jnp.broadcast_to(block[:, col0 + c:col0 + c + 1], (SUB, HALF)) for c in range(SUB)]


def invert_factor(work, inv_ref):
    rows = lax.broadcasted_iota(jnp.int32, (SUB, HALF), 0)
    left, right = row_blocks(work, 0)
    for r in range(0, HALF, SUB):
        more = r + SUB < HALF
        cols = lanes(left, r)
        if more:
            next_left, next_right = row_blocks(work, r + SUB)
            below = lanes(next_left, r)
        pivots = cols[0]
        for p in range(SUB):
            inv = 1.0 / cols[p][p:p + 1, :]
            fac = jnp.where(rows > p, cols[p] * inv, 0.0)
            left_row, right_row = left[p:p + 1, :], right[p:p + 1, :]
            left, right = left - fac * left_row, right - fac * right_row
            if more:
                low = below[p] * inv
                next_left, next_right = next_left - low * left_row, next_right - low * right_row
            for c in range(p + 1, SUB):
                entry = cols[c][p:p + 1, :]
                cols[c] = cols[c] - fac * entry
                if more:
                    below[c] = below[c] - low * entry
            pivots = jnp.where(rows == p, cols[p], pivots)
        scale = lax.rsqrt(pivots)
        left, right = left * scale, right * scale
        inv_ref[r:r + SUB, :] = right
        if r + 2 * SUB < HALF:
            upd = dot(left, jnp.concatenate([left, right], axis=1), ((0,), (0,)))
            work[r + 2 * SUB:, :] = work[r + 2 * SUB:, :] - upd[r + 2 * SUB:, :]
        if more:
            left, right = next_left, next_right


def eye(n):
    rows = lax.broadcasted_iota(jnp.int32, (n, n), 0)
    return jnp.where(rows == lax.broadcasted_iota(jnp.int32, (n, n), 1), 1.0, 0.0).astype(F32)


def factor(up, inv, work, small, n):
    panels = n // PANEL
    first, carry = small.at[0], small.at[1]

    def step(t, _):
        k, odd = t // 2, lax.rem(t, 2)
        r0 = pl.multiple_of(t * HALF, HALF)
        r1 = pl.multiple_of(t * HALF + HALF * (1 - odd), HALF)
        work[:, :HALF] = up[pl.ds(r0, HALF), pl.ds(r0, HALF)]
        work[:, HALF:] = eye(HALF)
        invert_factor(work, first)

        @pl.when(odd == 0)
        def _():
            w1 = first[...]
            inv[k] = jnp.zeros((PANEL, PANEL), F32)
            inv[k, :HALF, :HALF] = w1
            u12 = dot(w1, up[pl.ds(r0, HALF), pl.ds(r1, HALF)])
            both = dot(u12, jnp.concatenate([u12, w1], axis=1), ((0,), (0,)))
            up[pl.ds(r1, HALF), pl.ds(r1, HALF)] = up[pl.ds(r1, HALF), pl.ds(r1, HALF)] - both[:, :HALF]
            carry[...] = both[:, HALF:]

        @pl.when(odd == 1)
        def _():
            w2 = first[...]
            inv[k, HALF:, HALF:] = w2
            inv[k, HALF:, :HALF] = -dot(w2, carry[...])

        for kk in range(panels):
            @pl.when(t == 2 * kk + 1)
            def _():
                a, b = kk * PANEL, (kk + 1) * PANEL
                up[a:b, b:] = dot(inv[kk], up[a:b, b:])
                for i in range(kk + 1, panels):
                    c = i * PANEL
                    up[c:c + PANEL, c:] = up[c:c + PANEL, c:] - dot(up[a:b, c:c + PANEL], up[a:b, c:], ((0,), (0,)))
        return 0

    lax.fori_loop(0, 2 * panels, step, 0)


def places():
    z, dp = lax.axis_index('tp'), lax.axis_index('dp')
    core, x, y = lax.rem(dp, 2), lax.rem(dp // 2, 2), dp // 4
    return z, dp, core, x, y


def z_peers(z):
    return (z + 1 - 2 * lax.rem(z, 2), z + 2 - 4 * (z // 2), 3 - z)


def plane_peers(z, dp, core, x, y):
    return ({'tp': z, 'dp': dp + 1 - 2 * core}, {'tp': z, 'dp': dp + 2 - 4 * x}, {'tp': z, 'dp': dp + 4 - 8 * y})


def meet(peers):
    barrier = pltpu.get_barrier_semaphore()
    for peer in peers:
        pl.semaphore_signal(barrier, inc=1, device_id=peer, device_id_type=MESH)
    pl.semaphore_wait(barrier, len(peers))


def starter(send_sem, recv_sem):
    count = [0]

    def start(src, dst, peer):
        i = count[0]
        count[0] += 1
        copy = pltpu.make_async_remote_copy(src_ref=src, dst_ref=dst, send_sem=send_sem.at[i], recv_sem=recv_sem.at[i], device_id=peer, device_id_type=MESH)
        copy.start()
        return copy

    return start


def at(base, size):
    return pl.ds(pl.multiple_of(base, 8), size)


def spans(rows, core, x, y):
    half, quart, eighth, sixt = rows // 2, rows // 4, rows // 8, rows // 16
    a1, b1 = x * eighth, quart + y * eighth
    return core * half, a1, b1, a1 + y * sixt, b1 + x * sixt


def plane_scatter(rows, part, acc, got, start, peers, where):
    _, _, core, x, y = where
    core_peer, x_peer, y_peer = peers
    half, quart, eighth, sixt = rows // 2, rows // 4, rows // 8, rows // 16
    own, a1, b1, a2, b2 = spans(rows, core, x, y)
    got_core, got_a, got_b, got_a2, got_b2 = got
    copy = start(part.at[at((1 - core) * half, half)], got_core, core_peer)
    yield
    copy.wait()
    acc[...] = part[at(own, half)] + got_core[...]
    copies = [start(acc.at[at((1 - x) * eighth, eighth)], got_a, x_peer), start(acc.at[at(quart + (1 - y) * eighth, eighth)], got_b, y_peer)]
    yield
    copies[0].wait()
    acc[at(a1, eighth)] = acc[at(a1, eighth)] + got_a[...]
    copies[1].wait()
    acc[at(b1, eighth)] = acc[at(b1, eighth)] + got_b[...]
    copies = [start(acc.at[at(a1 + (1 - y) * sixt, sixt)], got_a2, y_peer), start(acc.at[at(b1 + (1 - x) * sixt, sixt)], got_b2, x_peer)]
    yield
    copies[0].wait()
    acc[at(a2, sixt)] = acc[at(a2, sixt)] + got_a2[...]
    copies[1].wait()
    acc[at(b2, sixt)] = acc[at(b2, sixt)] + got_b2[...]


def plane_gather(rows, full, start, peers, where):
    _, _, core, x, y = where
    core_peer, x_peer, y_peer = peers
    half, eighth, sixt = rows // 2, rows // 8, rows // 16
    own, a1, b1, a2, b2 = spans(rows, core, x, y)
    for sizes in (((a2, sixt, y_peer), (b2, sixt, x_peer)), ((a1, eighth, x_peer), (b1, eighth, y_peer)), ((0, half, core_peer),)):
        copies = []
        for base, size, peer in sizes:
            ref = full.at[:, at(own + base, size)]
            copies.append(start(ref, ref, peer))
        yield
        for copy in copies:
            copy.wait()


def in_turn(chunks):
    chunks = list(chunks)
    while chunks:
        chunks = [chunk for chunk in chunks if next(chunk, chunks) is not chunks]


def wait_all(copies):
    for copy in copies:
        copy.wait()


def sum_chunk(rows, part, acc, full, got, got_z, start, peers, z_peer, where):
    z, _, core, x, y = where
    yield from plane_scatter(rows, part, acc, got, start, peers, where)
    own, _, _, a2, b2 = spans(rows, core, x, y)
    share = rows // 64
    copies = []
    for k, piece in enumerate((a2, b2)):
        for j, peer in enumerate(z_peer):
            copies.append(start(acc.at[at(piece + peer['tp'] * share, share)], got_z.at[2 * j + k], peer))
    yield
    wait_all(copies)
    copies = []
    for k, piece in enumerate((a2, b2)):
        mine = piece + z * share
        full[0, at(own + mine, share)] = (acc[at(mine, share)] + got_z[k]) + (got_z[2 + k] + got_z[4 + k])
        ref = full.at[0, at(own + mine, share)]
        copies += [start(ref, ref, peer) for peer in z_peer]
    yield
    wait_all(copies)
    yield from plane_gather(rows, full, start, peers, where)


CHUNKS = 4


def sum_kernel(rows, part, out, acc, full, g0, g1, g2, g3, g4, got_z, send_sem, recv_sem, out_sem):
    where = places()
    z, dp = where[:2]
    peers = plane_peers(*where)
    z_peer = [{'tp': p, 'dp': dp} for p in z_peers(z)]
    meet(list(peers) + z_peer)
    start = starter(send_sem, recv_sem)
    size = rows // CHUNKS
    in_turn(sum_chunk(size, part.at[c * size:(c + 1) * size], acc.at[c], full.at[:, c * size:(c + 1) * size],
                      [g.at[c] for g in (g0, g1, g2, g3, g4)], got_z.at[c], start, peers, z_peer, where) for c in range(CHUNKS))
    copy = pltpu.make_async_copy(full, out, out_sem)
    copy.start()
    copy.wait()


def stack_kernel(rows, part, out, acc, mine, g0, g1, g2, g3, g4, send_sem, recv_sem, out_sem):
    where = places()
    z, dp, core, x, y = where
    peers = plane_peers(*where)
    z_peer = [{'tp': p, 'dp': dp} for p in z_peers(z)]
    meet(list(peers) + z_peer)
    start = starter(send_sem, recv_sem)
    in_turn([plane_scatter(rows, part, acc.at[0], [g.at[0] for g in (g0, g1, g2, g3, g4)], start, peers, where)])
    _, _, _, a2, b2 = spans(rows, core, x, y)
    sixt = rows // 16
    mine[z, :sixt] = acc[0, at(a2, sixt)]
    mine[z, sixt:] = acc[0, at(b2, sixt)]
    wait_all([start(mine.at[z], mine.at[z], peer) for peer in z_peer])
    copy = pltpu.make_async_copy(mine, out, out_sem)
    copy.start()
    copy.wait()


def spread_kernel(rows, mine, out, full, send_sem, recv_sem, out_sem):
    where = places()
    _, _, core, x, y = where
    peers = plane_peers(*where)
    meet(peers)
    own, _, _, a2, b2 = spans(rows, core, x, y)
    sixt = rows // 16
    full[:, at(own + a2, sixt)] = mine[:, :sixt]
    full[:, at(own + b2, sixt)] = mine[:, sixt:]
    start = starter(send_sem, recv_sem)
    in_turn(plane_gather(rows, full.at[c:c + 1], start, peers, where) for c in range(4))
    copy = pltpu.make_async_copy(full, out, out_sem)
    copy.start()
    copy.wait()


def scatter_scratch(chunks, rows):
    return [pltpu.VMEM((chunks, rows // d, BLOCK), F32) for d in (2, 8, 8, 16, 16)]


def comm_call(body, rows, operand, out_shape, scratch, copies, ident):
    return pl.pallas_call(
        functools.partial(body, rows),
        out_shape=jax.ShapeDtypeStruct(out_shape, F32),
        in_specs=[pl.BlockSpec(memory_space=pltpu.VMEM)],
        out_specs=pl.BlockSpec(memory_space=pl.ANY),
        scratch_shapes=scratch + [pltpu.SemaphoreType.DMA((copies,)), pltpu.SemaphoreType.DMA((copies,)), pltpu.SemaphoreType.DMA],
        compiler_params=pltpu.CompilerParams(collective_id=ident, has_side_effects=True, vmem_limit_bytes=24 * MIB),
        cost_estimate=pl.CostEstimate(flops=rows * 2000, bytes_accessed=80_000_000, transcendentals=0),
    )(operand)


def sum_all(part, ident):
    rows = part.shape[0]
    size = rows // CHUNKS
    scratch = [pltpu.VMEM((CHUNKS, size // 2, BLOCK), F32), pltpu.VMEM((1, rows, BLOCK), F32)] + scatter_scratch(CHUNKS, size) + [pltpu.VMEM((CHUNKS, 6, size // 64, BLOCK), F32)]
    return comm_call(sum_kernel, rows, part, (1, rows, BLOCK), scratch, 22 * CHUNKS, ident)


def stack_planes(part, ident):
    rows = part.shape[0]
    scratch = [pltpu.VMEM((1, rows // 2, BLOCK), F32), pltpu.VMEM((4, rows // 8, BLOCK), F32)] + scatter_scratch(1, rows)
    return comm_call(stack_kernel, rows, part, (4, rows // 8, BLOCK), scratch, 8, ident)


def spread_planes(mine, ident):
    rows = mine.shape[1] * 8
    return comm_call(spread_kernel, rows, mine, (4, rows, BLOCK), [pltpu.VMEM((4, rows, BLOCK), F32)], 20, ident)


def lower_back(up, inv, x_ref, x0, base):
    for k in range(PAIR // PANEL - 1, -1, -1):
        a, b = k * PANEL, (k + 1) * PANEL
        v = base(a, b)
        if b < PAIR:
            v = v - jnp.sum(up[a:b, b:PAIR] * x_ref[0:1, x0 + b:x0 + PAIR], axis=1, keepdims=True)
        x_ref[0:1, x0 + a:x0 + b] = jnp.sum(inv[k] * v, axis=0, keepdims=True)


def fetch_half(planes, stage, sems, first):
    copies = [pltpu.make_async_copy(planes.at[first + i], stage.at[i], sems.at[i]) for i in range(2)]
    for copy in copies:
        copy.start()
    return copies


def fill_half(copies, stage, up, ridge):
    wait_all(copies)
    diag = eye(BLOCK) * ridge
    for i in range(2):
        a, b = i * BLOCK, (i + 1) * BLOCK
        up[a:b, a:b] = stage[i, :BLOCK] + diag
        up[a:b, PAIR:] = stage[i, PAIR:].T


def low_kernel(planes, ridge, up, inv, stage, work, small, sems):
    fill_half(fetch_half(planes, stage, sems, 0), stage, up, ridge[0, 0])
    up[:BLOCK, BLOCK:PAIR] = stage[0, BLOCK:PAIR] + stage[1, BLOCK:PAIR]
    factor(up, inv, work, small, PAIR)


def high_kernel(planes, ridge, up_low, inv_low, cross, design, x_ref, fits, stage, mid, up, inv, work, small, rows, sems):
    copies = fetch_half(planes, stage, sems, 2)
    fetch = pltpu.make_async_copy(design, rows, sems.at[2])
    fetch.start()
    for j in range(2):
        mid[:, j * BLOCK:(j + 1) * BLOCK] = cross[0, j * PAIR:(j + 1) * PAIR, :]
    mid[:, PAIR:] = up_low[:, PAIR:]
    panels = PAIR // PANEL
    for k in range(panels):
        a, b = k * PANEL, (k + 1) * PANEL
        mid[a:b, :PAIR] = dot(inv_low[k], mid[a:b, :PAIR])
        for i in range(k + 1, panels):
            c = i * PANEL
            mid[c:c + PANEL, :PAIR] = mid[c:c + PANEL, :PAIR] - dot(up_low[a:b, c:c + PANEL], mid[a:b, :PAIR], ((0,), (0,)))
    fill_half(copies, stage, up, ridge[0, 0])
    up[:BLOCK, BLOCK:PAIR] = cross[0, 2 * PAIR:2 * PAIR + BLOCK]
    for i in range(panels):
        c = i * PANEL
        up[c:c + PANEL, c:] = up[c:c + PANEL, c:] - dot(mid[:, c:c + PANEL], mid[:, c:], ((0,), (0,)))
    factor(up, inv, work, small, PAIR)
    lower_back(up, inv, x_ref, PAIR, lambda a, b: up[a:b, PAIR:PAIR + 1])
    lower_back(up_low, inv_low, x_ref, 0, lambda a, b: up_low[a:b, PAIR:PAIR + 1] - jnp.sum(
        mid[a:b, :PAIR] * x_ref[0:1, PAIR:], axis=1, keepdims=True))
    fetch.wait()
    z = lax.axis_index('tp')
    x = [x_ref[0:1, pl.ds(pl.multiple_of(z * BLOCK + c * HALF, HALF), HALF)] for c in range(BLOCK // HALF)]
    group = 8

    def fit_rows(g, _):
        lines = []
        for r in range(group):
            base = pl.multiple_of((g * group + r) * HALF, HALF)
            t = sum(rows[pl.ds(base, HALF), c * HALF:(c + 1) * HALF] * x[c] for c in range(BLOCK // HALF))
            lines.append(jnp.sum(t.T, axis=0, keepdims=True))
        fits[pl.ds(pl.multiple_of(g * group, group), group), :] = jnp.concatenate(lines, axis=0)
        return 0

    lax.fori_loop(0, fits.shape[0] // group, fit_rows, 0)


VM = pl.BlockSpec(memory_space=pltpu.VMEM)
SM = pl.BlockSpec(memory_space=pltpu.SMEM)
HB = pl.BlockSpec(memory_space=pl.ANY)
PANELS_SHAPE = (PAIR // PANEL, PANEL, PANEL)


def factor_low(planes, ridge):
    rows = planes.shape[1]
    return pl.pallas_call(
        low_kernel,
        out_shape=(jax.ShapeDtypeStruct((PAIR, PAIR + EXTRA), F32), jax.ShapeDtypeStruct(PANELS_SHAPE, F32)),
        in_specs=[HB, SM],
        out_specs=(VM, VM),
        scratch_shapes=[pltpu.VMEM((2, rows, BLOCK), F32), pltpu.VMEM((HALF, 2 * HALF), F32), pltpu.VMEM((2, HALF, HALF), F32), pltpu.SemaphoreType.DMA((2,))],
        compiler_params=pltpu.CompilerParams(vmem_limit_bytes=24 * MIB),
        cost_estimate=pl.CostEstimate(flops=40_000_000_000, bytes_accessed=10_000_000, transcendentals=0),
        name="factor_low",
    )(planes, ridge)


def factor_high(planes, ridge, up_low, inv_low, cross, design_blk):
    rows = planes.shape[1]
    lines = design_blk.shape[0] // HALF
    return pl.pallas_call(
        high_kernel,
        out_shape=(jax.ShapeDtypeStruct((1, 2 * PAIR), F32), jax.ShapeDtypeStruct((lines, HALF), F32)),
        in_specs=[HB, SM, VM, VM, VM, HB],
        out_specs=(VM, VM),
        scratch_shapes=[
            pltpu.VMEM((2, rows, BLOCK), F32),
            pltpu.VMEM((PAIR, PAIR + EXTRA), F32),
            pltpu.VMEM((PAIR, PAIR + EXTRA), F32),
            pltpu.VMEM(PANELS_SHAPE, F32),
            pltpu.VMEM((HALF, 2 * HALF), F32),
            pltpu.VMEM((2, HALF, HALF), F32),
            pltpu.VMEM(design_blk.shape, F32),
            pltpu.SemaphoreType.DMA((3,)),
        ],
        compiler_params=pltpu.CompilerParams(vmem_limit_bytes=42 * MIB),
        cost_estimate=pl.CostEstimate(flops=50_000_000_000, bytes_accessed=10_000_000, transcendentals=0),
        name="factor_high",
    )(planes, ridge, up_low, inv_low, cross, design_blk)


CROSS_ROWS = 2048


def cross_kernel(early, has_pair, has_prev, own, mate_lo, mate_hi, far_c, far_d, *refs):
    out, panel = refs[-2:]
    z = lax.axis_index('tp')
    mate, even, other = z_peers(z)

    def column(index):
        return pl.ds(pl.multiple_of(index * BLOCK, BLOCK), BLOCK)

    @pl.when(pl.program_id(0) == 0)
    def _():
        out[...] = refs[-3][...] if has_prev else jnp.zeros((CROSS_ROWS, BLOCK), F32)
        if has_pair:
            out[2 * PAIR:2 * PAIR + BLOCK] += refs[0][...]

    full = 1 if early else 0
    panel[:, column(z)] = own[...]
    panel[:, column(even)] = far_d[...]
    panel[:, column(other)] = far_c[...]

    @pl.when(z < 2)
    def _():
        panel[:, column(mate)] = mate_lo[...]

    @pl.when(z >= 2)
    def _():
        panel[:, column(mate)] = mate_hi[...]

    @pl.when((z == full) | (z >= 2))
    def _():
        def row_block(i, _):
            low = panel[:, column(i)]
            for j in range(2):
                a = pl.multiple_of(j * PAIR + i * BLOCK, BLOCK)
                hi = panel[:, PAIR + j * BLOCK:PAIR + (j + 1) * BLOCK]
                out[pl.ds(a, BLOCK)] += dot(low, hi, ((0,), (0,)))
            return 0

        lax.fori_loop(jnp.where(z < 2, 0, full), jnp.where(z < 2, 2, full + 1), row_block, 0)

    if early:
        @pl.when(z >= 2)
        def _():
            out[2 * PAIR:2 * PAIR + BLOCK] += dot(panel[:, PAIR:PAIR + BLOCK], panel[:, PAIR + BLOCK:], ((0,), (0,)))


def cross_gram(early, row0, own, mate_lo, mate_hi, far_c, far_d, prev=None, pair=None):
    rows = far_c.shape[0]
    tile = 256
    steps = rows // tile
    shift = row0 // tile
    near = pl.BlockSpec((tile, BLOCK), lambda i: (i + shift, 0))
    far = pl.BlockSpec((tile, BLOCK), lambda i: (i, 0))
    extras = [a for a in (pair, prev) if a is not None]

    return pl.pallas_call(
        functools.partial(cross_kernel, early, pair is not None, prev is not None),
        out_shape=jax.ShapeDtypeStruct((CROSS_ROWS, BLOCK), F32),
        grid=(steps,),
        in_specs=[near, near, near, far, far] + [pl.BlockSpec(a.shape, lambda i: (0, 0)) for a in extras],
        out_specs=pl.BlockSpec((CROSS_ROWS, BLOCK), lambda i: (0, 0)),
        scratch_shapes=[pltpu.VMEM((tile, 2 * PAIR), F32)],
        compiler_params=pltpu.CompilerParams(dimension_semantics=("arbitrary",), vmem_limit_bytes=24 * MIB),
        cost_estimate=pl.CostEstimate(flops=rows * 6_000_000, bytes_accessed=rows * 8000, transcendentals=0),
        name="cross_gram",
    )(own, mate_lo, mate_hi, far_c, far_d, *extras)


def own_kernel(design, target, part):
    @pl.when(pl.program_id(0) == 0)
    def _():
        part[...] = jnp.zeros_like(part)

    part[:BLOCK] += dot(design[...], design[...], ((0,), (0,)))
    part[PAIR:PAIR + 1] += dot(target[0], design[...])


def own_gram(design_blk, target_blk):
    rows = design_blk.shape[0]
    tile = 256
    return pl.pallas_call(
        own_kernel,
        out_shape=jax.ShapeDtypeStruct((PAIR + EXTRA, BLOCK), F32),
        grid=(rows // tile,),
        in_specs=[pl.BlockSpec((tile, BLOCK), lambda i: (i, 0)), pl.BlockSpec((1, 1, tile), lambda i: (i, 0, 0))],
        out_specs=pl.BlockSpec((PAIR + EXTRA, BLOCK), lambda i: (0, 0)),
        compiler_params=pltpu.CompilerParams(dimension_semantics=("arbitrary",), vmem_limit_bytes=24 * MIB),
        cost_estimate=pl.CostEstimate(flops=30_000_000_000, bytes_accessed=13_000_000, transcendentals=0),
        name="own_gram",
    )(design_blk, jnp.reshape(target_blk, (rows // tile, 1, tile)))


def pair_kernel(low, near, mate, head, out, panel):
    z = lax.axis_index('tp')
    r = BLOCK if low else 0

    @pl.when(pl.program_id(0) == 0)
    def _():
        out[...] = head[...] if out.shape == head.shape else jnp.zeros_like(out)

    @pl.when(z < 2 if low else z >= 2)
    def _():
        odd = lax.rem(z, 2)
        panel[:, pl.ds(pl.multiple_of(odd * BLOCK, BLOCK), BLOCK)] = near[...]
        panel[:, pl.ds(pl.multiple_of((1 - odd) * BLOCK, BLOCK), BLOCK)] = mate[...]
        out[r:r + BLOCK] += dot(panel[:, :BLOCK], panel[:, BLOCK:], ((0,), (0,)))


def pair_gram(low, near_rows, mate, head, row0=0):
    rows = mate.shape[0]
    tile = 256
    shift = row0 // tile
    out_rows = PAIR + EXTRA if low else BLOCK
    return pl.pallas_call(
        functools.partial(pair_kernel, low),
        out_shape=jax.ShapeDtypeStruct((out_rows, BLOCK), F32),
        grid=(rows // tile,),
        in_specs=[
            pl.BlockSpec((tile, BLOCK), lambda i: (i + shift, 0)),
            pl.BlockSpec((tile, BLOCK), lambda i: (i, 0)),
            pl.BlockSpec(head.shape, lambda i: (0, 0)),
        ],
        out_specs=pl.BlockSpec((out_rows, BLOCK), lambda i: (0, 0)),
        scratch_shapes=[pltpu.VMEM((tile, PAIR), F32)],
        compiler_params=pltpu.CompilerParams(dimension_semantics=("arbitrary",), vmem_limit_bytes=24 * MIB),
        cost_estimate=pl.CostEstimate(flops=rows * 3_000_000, bytes_accessed=rows * 6000, transcendentals=0),
        name="pair_gram",
    )(near_rows, mate, head)


def residual_kernel(fit, target, out, got, send_sem, recv_sem):
    z, dp = lax.axis_index('tp'), lax.axis_index('dp')
    peers = [{'tp': p, 'dp': dp} for p in z_peers(z)]
    meet(peers)
    start = starter(send_sem, recv_sem)
    wait_all([start(fit, got.at[j], peer) for j, peer in enumerate(peers)])
    out[...] = target[...] - ((fit[...] + got[0]) + (got[1] + got[2]))


def residual(fits, target_tile):
    return pl.pallas_call(
        residual_kernel,
        out_shape=jax.ShapeDtypeStruct(target_tile.shape, F32),
        in_specs=[VM, VM],
        out_specs=VM,
        scratch_shapes=[pltpu.VMEM((3,) + target_tile.shape, F32), pltpu.SemaphoreType.DMA((3,)), pltpu.SemaphoreType.DMA((3,))],
        compiler_params=pltpu.CompilerParams(collective_id=3, has_side_effects=True),
        cost_estimate=pl.CostEstimate(flops=3_000_000_000, bytes_accessed=1_000_000, transcendentals=0),
        name="residual",
    )(fits, target_tile)


EDGES = (0, 512, 1536, 2048)


def solution(mesh):
    col_ways, row_ways = mesh.shape['tp'], mesh.shape['dp']

    def swap(block, one, two):
        pairs = [(s * row_ways + d, t * row_ways + d) for s, t in ((one, two), (two, one)) for d in range(row_ways)]
        return lax.ppermute(block, ('tp', 'dp'), pairs)

    def local_fit(design_blk, target_blk, ridge):
        rows_dev, _ = design_blk.shape
        quarter_rows = rows_dev // col_ways
        z = lax.axis_index('tp')

        def piece(array, index):
            return lax.dynamic_slice_in_dim(array, index * quarter_rows, quarter_rows)

        to_mate = piece(design_blk, z ^ 1)
        to_mate, design_b = lax.optimization_barrier((to_mate, design_blk))
        low_a = swap(to_mate, 0, 1)
        to_third = piece(design_b, z ^ 3)
        to_third, design_b = lax.optimization_barrier((to_third, design_b))
        to_even = piece(design_b, z ^ 2)
        low_b = swap(to_third, 0, 1)
        near_c = swap(to_third, 1, 2)
        near_d = swap(to_even, 1, 3)
        high_a = swap(to_mate, 2, 3)
        to_third_b, to_even_b, design_b = lax.optimization_barrier((to_third, to_even, design_b))
        own = piece(design_b, z)
        chunks = [(to_third_b[i:j], to_even_b[i:j]) for i, j in zip(EDGES, EDGES[1:])]
        late_b = to_third_b[EDGES[1]:]
        part = own_gram(design_b, target_blk)
        part = pair_gram(True, own, low_a, part)
        low_a, low_b, near_c, near_d, part, chunks = lax.optimization_barrier(
            (low_a, low_b, near_c, near_d, part, chunks))
        far_c, far_d = [], []

        def send_late(pieces):
            far_c.append(swap(pieces[0], 0, 3))
            far_d.append(swap(pieces[1], 0, 2))

        send_late(chunks[0])
        high_b0 = swap(chunks[0][0], 2, 3)
        part = pair_gram(True, to_even, low_b, part)
        mine = stack_planes(part, 1)
        mine, late_b, chunks = lax.optimization_barrier((mine, late_b, chunks))
        send_late(chunks[1])
        high_b1 = swap(late_b, 2, 3)
        send_late(chunks[2])
        planes = spread_planes(mine, 2)
        ridge_cell = jnp.reshape(ridge, (1, 1))
        up_low, inv_low = factor_low(planes, ridge_cell)
        own_b, near_c, up_low = lax.optimization_barrier((own, near_c, up_low))
        cross = cross_gram(True, 0, own_b, low_a, high_a, near_c, near_d)
        cross = cross_gram(False, EDGES[0], own_b, low_a, high_a, far_c[0], far_d[0], cross)
        pair_high = pair_gram(False, to_even, high_b0, jnp.zeros((8, BLOCK), F32))
        cross = cross_gram(False, EDGES[1], own_b, low_a, high_a, far_c[1], far_d[1], cross)
        high_b1, cross = lax.optimization_barrier((high_b1, cross))
        pair_high = pair_gram(False, to_even, high_b1, pair_high, EDGES[1])
        cross = cross_gram(False, EDGES[2], own_b, low_a, high_a, far_c[2], far_d[2], cross, pair_high)
        cross = sum_all(cross, 4)
        x_row, fits = factor_high(planes, ridge_cell, up_low, inv_low, cross, design_b)
        left = residual(fits, jnp.reshape(target_blk, (rows_dev // HALF, HALF)))
        return x_row[0], jnp.reshape(left, (rows_dev,))

    return jax.shard_map(local_fit, mesh=mesh, in_specs=(P('dp', 'tp'), P('dp'), P()), out_specs=(P(), P('dp')), check_vma=False)
```
